32 devices in a mesh: groups: 2 (over y), seq: 4 (over z), head: 2 (over x), sub: 2 (over core).
Axes of the slice: x: 2, y: 2, z: 4, core: 2. Of those that a mesh axis runs over, the one named last changes fastest.
Arguments:
- queries: bfloat16 [32, 64, 8192], P(('groups', 'seq'), None, 'head'), parts along dimension 0, may hold values from -6 to 6
- new_kv: bfloat16 [32, 64, 2, 1024], P(('groups', 'seq'), None, None, 'head'), parts along dimension 0, may hold values from -6 to 6
- kv_pages: bfloat16 [336, 2, 128, 1024], P(('groups', 'seq', 'sub'), None, None, 'head'), parts along dimension 0, may hold values from -6 to 6
- page_table: int32 [32, 16], P('groups'), parts along dimension 0, may hold values from -1 to 167, as said below
- cached_len: int32 [32], P('groups'), parts along dimension 0, may hold values from 1 to 2048, as said below
- is_prefill: int32 [32], P('groups'), parts along dimension 0, may hold values from 0 to 1, as said below
Outputs:
- attended: bfloat16 [32, 64, 8192], P(('groups', 'seq'), None, 'head'), parts along dimension 0
The draws below stay inside these ranges and needn't reach their ends.
There are 2 independent parts, one for each index of `groups`. The reference program is written for one: setup_inputs(seed, part) draws one part's arguments, and reference() takes and returns one part's arrays. A program takes and returns all parts, laid end to end along the dimension named above; each array names one. Nothing has to cross between parts.
Inputs may be any that keep to these rules, and one draw needn't show every extreme that they name: `page_table`: entry [s, p] is the page number of page p of sequence s for p < ceil(cached_len[s] / 128) and -1 after; page number q lies on owner q // 21 (owner index = seq index * 2 + sub index) in its slot q % 21. Listing the pages of all sequences in order of sequence and page as t = 0, 1, ..., page t has owner (t + c) % 8 and slot (t + c) // 8 for one drawn c. No owner holds more than 8 page of the 4 sequences of one seq shard, and some owner holds exactly 8. `cached_len`: A decode sequence has 1 to 4 cache pages, a prefill sequence 8 to 16; all 4 sequences of one drawn seq shard are prefill sequences with 16 pages. `is_prefill`: exactly 8 sequences are prefill sequences.
All inputs are finite; a program needn't handle non-finite values.
Results may differ from the reference program's by a relative error of at most 0.014.
Values may be sent and summed in bfloat16 or wider, within the bound.
No kernel may reach another device: no remote copies, remote signals or barrier semaphores. Data moves between devices by JAX's collectives and lax.ppermute only.
A program may use at most 64 MiB of HBM per device.

```python
import jax
import jax.numpy as jnp
from jax import lax

HQ = 64
KVH = 8
HD = 128
PAGE = 128
MAXP = 16
DEC_MAXP = 4
QROWS = 64
SEQ_DEV = 4
SEQS = 16
PREFILL = 8
OWNERS = 8
PAGES_DEV = 21


def page_layout(key):
    heavy_key = jax.random.fold_in(key, 101)
    order_key = jax.random.fold_in(key, 102)
    long_key = jax.random.fold_in(key, 103)
    short_key = jax.random.fold_in(key, 104)
    tail_key = jax.random.fold_in(key, 105)
    rotate_key = jax.random.fold_in(key, 106)
    shard_total = SEQS // SEQ_DEV
    heavy = jax.random.randint(heavy_key, (), 0, shard_total)
    seq_ids = jnp.arange(SEQS, dtype=jnp.int32)
    in_heavy = seq_ids // SEQ_DEV == heavy
    shuffled = jax.random.permutation(order_key, SEQS).astype(jnp.int32)
    keyed = jnp.where(in_heavy, -1, shuffled)
    standing = jnp.sum((keyed[None, :] < keyed[:, None]).astype(jnp.int32), axis=1)
    prefill = standing < PREFILL
    long_pages = jax.random.randint(long_key, (SEQS,), MAXP // 2, MAXP + 1)
    short_pages = jax.random.randint(short_key, (SEQS,), 1, DEC_MAXP + 1)
    page_total = jnp.where(in_heavy, MAXP, jnp.where(prefill, long_pages, short_pages)).astype(jnp.int32)
    cached = (page_total - 1) * PAGE + jax.random.randint(tail_key, (SEQS,), 1, PAGE + 1)
    first_page = jnp.cumsum(page_total) - page_total
    rotation = jax.random.randint(rotate_key, (), 0, OWNERS)
    page_ids = jnp.arange(MAXP, dtype=jnp.int32)
    linear = first_page[:, None] + page_ids[None, :] + rotation
    number = linear % OWNERS * PAGES_DEV + linear // OWNERS
    table_rows = jnp.where(page_ids[None, :] < page_total[:, None], number, -1)
    return (table_rows.astype(jnp.int32), cached.astype(jnp.int32), prefill.astype(jnp.int32))


def draw_page_table(key, part):
    return page_layout(key)[0]


def draw_cached_len(key, part):
    return page_layout(key)[1]


def draw_is_prefill(key, part):
    return page_layout(key)[2]


def draw_queries(key, part):
    shape = (SEQS, QROWS, HQ * HD)
    values = jnp.clip(jax.random.normal(jax.random.fold_in(key, 11), shape, jnp.float32), -5.0, 5.0)
    return values.astype(jnp.bfloat16)


def draw_kv_pages(key, part):
    shape = (PAGES_DEV * OWNERS, 2, PAGE, KVH * HD)
    values = jnp.clip(jax.random.normal(jax.random.fold_in(key, 12), shape, jnp.float32), -5.0, 5.0)
    return values.astype(jnp.bfloat16)


def block_levels(stream_key, extent, pieces, least, largest):
    loudness, own = 1.0, jax.random.fold_in(stream_key, 6)
    for dim, blocks in pieces:
        steps = jnp.exp(jax.random.uniform(jax.random.fold_in(own, dim), (blocks,), jnp.float32, least / len(pieces), largest / len(pieces)))
        loudness = loudness * jnp.repeat(steps, extent[dim] // blocks).reshape([-1 if axis == dim else 1 for axis in range(len(extent))])
    return loudness


def normal_values(rng, shape, scale, bound, pieces=(), kind=jnp.bfloat16):
    level = block_levels(rng, shape, pieces, -0.22, 0.18) if pieces else 1.0
    values = jax.random.normal(rng, shape, jnp.float32) * scale * level
    return jnp.minimum(jnp.maximum(values, -bound), bound).astype(kind)


def setup_inputs(seed: int = 0, part: int = 0) -> dict:
    splits = jax.random.split(jax.random.key(seed), 7)
    own_keys = jax.random.split(jax.random.fold_in(splits[6], part), 7)
    return {
        "queries": draw_queries(jax.random.fold_in(jax.random.fold_in(splits[6], part), 71), part),
        "new_kv": normal_values(own_keys[1], (SEQS, QROWS, 2, KVH * HD), 1.0, 6.0, ((0, 4), (3, 2))),
        "kv_pages": draw_kv_pages(jax.random.fold_in(jax.random.fold_in(splits[6], part), 71), part),
        "page_table": draw_page_table(jax.random.fold_in(jax.random.fold_in(splits[6], part), 71), part),
        "cached_len": draw_cached_len(jax.random.fold_in(jax.random.fold_in(splits[6], part), 71), part),
        "is_prefill": draw_is_prefill(jax.random.fold_in(jax.random.fold_in(splits[6], part), 71), part),
    }


NEG_FILL = -1e30


def reference(queries, new_kv, kv_pages, page_table, cached_len, is_prefill):
    group_size = HQ // KVH
    score_scale = HD ** -0.5
    positions = jnp.arange(MAXP * PAGE, dtype=jnp.int32)
    row_ids = jnp.arange(QROWS, dtype=jnp.int32)
    causal = row_ids[None, :] <= row_ids[:, None]

    def one_sequence(inputs):
        query_rows, fresh_rows, table_row, length, flag = inputs
        fetched = jnp.take(kv_pages, jnp.maximum(table_row, 0).astype(jnp.int32), axis=0)
        cache_keys = fetched[:, 0].reshape(MAXP * PAGE, KVH, HD).astype(jnp.float32)
        cache_values = fetched[:, 1].reshape(MAXP * PAGE, KVH, HD).astype(jnp.float32)
        cache_valid = positions < length
        live_row = (flag == 1) | (row_ids == 0)
        query_heads = query_rows.reshape(QROWS, KVH, group_size, HD).astype(jnp.float32)
        fresh_keys = fresh_rows[:, 0].reshape(QROWS, KVH, HD).astype(jnp.float32)
        fresh_values = fresh_rows[:, 1].reshape(QROWS, KVH, HD).astype(jnp.float32)
        fresh_valid = causal & live_row[:, None]
        cache_scores = jnp.einsum("rkgd,nkd->kgrn", query_heads, cache_keys) * score_scale
        fresh_scores = jnp.einsum("rkgd,jkd->kgrj", query_heads, fresh_keys) * score_scale
        cache_mask = cache_valid[None, None, None, :]
        fresh_mask = fresh_valid[None, None, :, :]
        peak = jnp.maximum(jnp.max(jnp.where(cache_mask, cache_scores, NEG_FILL), axis=-1),
                           jnp.max(jnp.where(fresh_mask, fresh_scores, NEG_FILL), axis=-1))
        cache_weights = jnp.where(cache_mask, jnp.exp(cache_scores - peak[..., None]), 0.0)
        fresh_weights = jnp.where(fresh_mask, jnp.exp(fresh_scores - peak[..., None]), 0.0)
        weight_sum = jnp.sum(cache_weights, axis=-1) + jnp.sum(fresh_weights, axis=-1)
        cache_rounded = lax.optimization_barrier(cache_weights.astype(jnp.bfloat16)).astype(jnp.float32)
        fresh_rounded = lax.optimization_barrier(fresh_weights.astype(jnp.bfloat16)).astype(jnp.float32)
        numerator = jnp.einsum("kgrn,nkd->kgrd", cache_rounded, cache_values)
        numerator = numerator + jnp.einsum("kgrj,jkd->kgrd", fresh_rounded, fresh_values)
        unused_rows = 1.0 - live_row.astype(jnp.float32)
        attended = numerator / (weight_sum + unused_rows[None, None, :])[..., None]
        attended = jnp.where(live_row[None, None, :, None], attended, 0.0)
        return jnp.transpose(attended, (2, 0, 1, 3)).reshape(QROWS, HQ * HD).astype(jnp.bfloat16)

    return lax.map(one_sequence, (queries, new_kv, page_table, cached_len, is_prefill))
```

```python
import jax
import jax.numpy as jnp
from jax import lax
from jax.experimental import pallas as pl
from jax.experimental.pallas import tpu as pltpu
from jax.sharding import PartitionSpec as P

HD = 128
PAGE = 128


NEG_FILL = -1e30


def partial_softmax(
    query_heads, cache_keys, cache_values, cache_valid, fresh_keys, fresh_values, fresh_valid
):
    score_scale = HD ** (-0.5)
    cache_scores = (
        jnp.einsum("rkgd,nkd->kgrn", query_heads, cache_keys, preferred_element_type=jnp.float32)
        * score_scale
    )
    fresh_scores = (
        jnp.einsum("rkgd,jkd->kgrj", query_heads, fresh_keys, preferred_element_type=jnp.float32)
        * score_scale
    )
    cache_mask = cache_valid[None, None, None, :]
    fresh_mask = fresh_valid[None, None, :, :]
    peak = jnp.maximum(
        jnp.max(jnp.where(cache_mask, cache_scores, NEG_FILL), axis=-1),
        jnp.max(jnp.where(fresh_mask, fresh_scores, NEG_FILL), axis=-1),
    )
    cache_weights = jnp.where(cache_mask, jnp.exp(cache_scores - peak[..., None]), 0.0)
    fresh_weights = jnp.where(fresh_mask, jnp.exp(fresh_scores - peak[..., None]), 0.0)
    weight_sum = jnp.sum(cache_weights, axis=-1) + jnp.sum(fresh_weights, axis=-1)
    numerator = jnp.einsum(
        "kgrn,nkd->kgrd",
        cache_weights.astype(jnp.bfloat16),
        cache_values,
        preferred_element_type=jnp.float32,
    )
    numerator = numerator + jnp.einsum(
        "kgrj,jkd->kgrd",
        fresh_weights.astype(jnp.bfloat16),
        fresh_values,
        preferred_element_type=jnp.float32,
    )
    return (peak, weight_sum, numerator)


def attend_all(
    query_block, fresh_block, received, fetch_index, page_here, lengths, live_rows, causal, fresh_on
):
    kv_width = received.shape[-1]
    heads_kv = kv_width // HD
    row_count = query_block.shape[1]
    group_size = query_block.shape[2] // kv_width
    page_count = fetch_index.shape[1]
    positions = jnp.arange(page_count * PAGE, dtype=jnp.int32)

    def one_sequence(inputs):
        query_rows, fresh_rows, index_row, here_row, length, live_row = inputs
        fetched = jnp.take(received, index_row, axis=0)
        cache_keys = fetched[:, 0].reshape(page_count * PAGE, heads_kv, HD)
        cache_values = fetched[:, 1].reshape(page_count * PAGE, heads_kv, HD)
        page_mask = jnp.broadcast_to(here_row[:, None], (page_count, PAGE)).reshape(
            page_count * PAGE
        )
        cache_valid = page_mask & (positions < length)
        query_heads = query_rows.reshape(row_count, heads_kv, group_size, HD)
        fresh_keys = fresh_rows[:, 0].reshape(row_count, heads_kv, HD)
        fresh_values = fresh_rows[:, 1].reshape(row_count, heads_kv, HD)
        fresh_valid = causal & live_row[:, None] & fresh_on
        return partial_softmax(
            query_heads,
            cache_keys,
            cache_values,
            cache_valid,
            fresh_keys,
            fresh_values,
            fresh_valid,
        )

    return lax.map(
        one_sequence, (query_block, fresh_block, fetch_index, page_here, lengths, live_rows)
    )


def finish(weight_sum, numerator, live_rows):
    unused_rows = 1.0 - live_rows.astype(jnp.float32)
    attended = numerator / (weight_sum + unused_rows[:, None, None, :])[..., None]
    attended = jnp.where(live_rows[:, None, None, :, None], attended, 0.0)
    seq_dev, heads_kv, group_size, row_count, head_dim = attended.shape
    return (
        jnp.transpose(attended, (0, 3, 1, 2, 4))
        .reshape(seq_dev, row_count, heads_kv * group_size * head_dim)
        .astype(jnp.bfloat16)
    )


def pages_travel(queries, new_kv, kv_pages, page_table, cached_len, is_prefill):
    seq_shards = lax.axis_size("seq")
    sub_count = lax.axis_size("sub")
    owners = seq_shards * sub_count
    seq_index = lax.axis_index("seq")
    core_index = lax.axis_index("sub")
    owner_self = seq_index * sub_count + core_index
    seq_dev, row_count, query_width = queries.shape
    pages_dev = kv_pages.shape[0]
    kv_width = kv_pages.shape[3]
    page_count = page_table.shape[1]
    entries = seq_dev * page_count
    capacity = (entries + owners - 1) // owners
    table_rows = page_table.reshape(seq_shards, entries)
    holder = jnp.where(table_rows >= 0, table_rows // pages_dev, -1)
    slot_of = jnp.where(table_rows >= 0, table_rows % pages_dev, 0)
    owned_here = holder == owner_self
    rank_among = jnp.cumsum(owned_here.astype(jnp.int32), axis=1) - 1
    picked = owned_here[:, :, None] & (
        rank_among[:, :, None] == jnp.arange(capacity, dtype=jnp.int32)[None, None, :]
    )
    send_slots = jnp.sum(jnp.where(picked, slot_of[:, :, None], 0), axis=1).reshape(
        seq_shards * capacity
    )
    first_seq = seq_index * seq_dev
    my_table = lax.dynamic_slice_in_dim(page_table, first_seq, seq_dev, 0)
    my_lengths = lax.dynamic_slice_in_dim(cached_len, first_seq, seq_dev, 0)
    my_flags = lax.dynamic_slice_in_dim(is_prefill, first_seq, seq_dev, 0)
    flat_table = my_table.reshape(entries)
    my_holder = jnp.where(flat_table >= 0, flat_table // pages_dev, -1)
    entry_order = jnp.arange(entries, dtype=jnp.int32)
    earlier = (my_holder[:, None] == my_holder[None, :]) & (
        entry_order[None, :] < entry_order[:, None]
    )
    my_rank = jnp.sum(earlier.astype(jnp.int32), axis=1)
    row_ids = jnp.arange(row_count, dtype=jnp.int32)
    live_rows = (my_flags[:, None] == 1) | (row_ids[None, :] == 0)
    causal = row_ids[None, :] <= row_ids[:, None]
    part_width = kv_width // sub_count
    split_pages = kv_pages.reshape(pages_dev, 2, PAGE, sub_count, part_width)
    chosen = jnp.take(split_pages, send_slots, axis=0).reshape(
        seq_shards, capacity, 2, PAGE, sub_count, part_width
    )
    outgoing = jnp.moveaxis(chosen, 4, 1).reshape(owners, capacity, 2, PAGE, part_width)
    received = lax.all_to_all(
        outgoing, ("seq", "sub"), split_axis=0, concat_axis=0, tiled=True
    ).reshape(owners * capacity, 2, PAGE, part_width)
    present = flat_table >= 0
    fetch_index = jnp.where(present, my_holder * capacity + my_rank, 0)
    query_part = query_width // sub_count
    my_queries = lax.dynamic_slice_in_dim(queries, core_index * query_part, query_part, 2)
    my_fresh = lax.dynamic_slice_in_dim(new_kv, core_index * part_width, part_width, 3)
    peak, weight_sum, numerator = attend_all(
        my_queries,
        my_fresh,
        received,
        fetch_index.reshape(seq_dev, page_count),
        present.reshape(seq_dev, page_count),
        my_lengths,
        live_rows,
        causal,
        core_index >= 0,
    )
    own_heads = finish(weight_sum, numerator, live_rows)
    return lax.all_gather(own_heads, "sub", axis=2, tiled=True)


LOG2E = 1.4426950408889634
LANES = 128
NO_KEY = -1e30


def page_plan(page_table, cached_len, is_prefill, shard, core, pages_dev, sub_count, picks):
    seqs, page_count = page_table.shape
    present = page_table >= 0
    owner = jnp.where(present, page_table // pages_dev, -1)
    slot = jnp.where(present, page_table % pages_dev, 0)
    page_ids = jnp.arange(page_count, dtype=jnp.int32)
    keys_here = jnp.clip(cached_len[:, None] - page_ids[None, :] * PAGE, 0, PAGE)
    before = page_ids[None, :] < page_ids[:, None]
    same = owner[:, :, None] == owner[:, None, :]
    rank = jnp.sum((same & before[None]).astype(jnp.int32), axis=2)
    cores = (core + jnp.arange(sub_count, dtype=jnp.int32)) % sub_count
    wanted = shard * sub_count + cores
    picked = (owner[:, None, None, :] == wanted[None, :, None, None]) & (
        rank[:, None, None, :] == jnp.arange(picks, dtype=jnp.int32)[None, None, :, None]
    )
    slots = jnp.sum(jnp.where(picked, slot[:, None, None, :], 0), axis=3)
    counts = jnp.sum(jnp.where(picked, keys_here[:, None, None, :], 0), axis=3)
    rows = jnp.concatenate(
        [
            slots.reshape(seqs, sub_count * picks),
            counts.reshape(seqs, sub_count * picks),
            is_prefill[:, None].astype(jnp.int32),
        ],
        axis=1,
    )
    return jnp.concatenate([jnp.stack([shard, core]).astype(jnp.int32), rows.reshape(-1)])


def lse_block(lse_tile, heads):
    lane = lax.broadcasted_iota(jnp.int32, lse_tile.shape, 1)
    high = lse_tile.astype(jnp.bfloat16)
    rest = lse_tile - high.astype(jnp.float32)
    middle = rest.astype(jnp.bfloat16)
    low = rest - middle.astype(jnp.float32)
    mixed = jnp.where(
        lane < heads,
        high.astype(jnp.float32),
        jnp.where(lane < 2 * heads, middle.astype(jnp.float32), low),
    )
    return mixed.astype(jnp.bfloat16)


def read_lse(block, heads):
    tile = block.astype(jnp.float32)
    return (
        tile
        + pltpu.roll(tile, LANES - heads, 1)
        + pltpu.roll(tile, LANES - 2 * heads, 1)
    )


def spread_lse(lse, heads):
    lane = lax.broadcasted_iota(jnp.int32, lse.shape, 1)
    return jnp.where(
        lane < heads,
        lse,
        jnp.where(lane < 2 * heads, pltpu.roll(lse, heads, 1), pltpu.roll(lse, 2 * heads, 1)),
    )


def partial_attention(
    plan, query, pages, twin_pages, fresh, *, offset, first, shards, seq_dev, picks, sub_count
):
    count, row_count, width = query.shape
    part_width = twin_pages.shape[3]
    heads_kv = part_width // HD
    heads = width // HD
    group = heads // heads_kv
    refs_per_seq = sub_count * picks
    record = 2 * refs_per_seq + 1
    scale = LOG2E * HD ** (-0.5)

    def entry(plan_ref, k, column):
        home = jnp.clip(plan_ref[0] + offset, 0, shards - 1)
        return plan_ref[2 + (home * seq_dev + first + k) * record + column]

    def body(plan_ref, query_ref, *rest):
        page_refs = rest[:refs_per_seq]
        fresh_refs = rest[refs_per_seq:-1]
        out_ref = rest[-1]
        k = pl.program_id(0)
        home = plan_ref[0] + offset
        counts = [entry(plan_ref, k, refs_per_seq + n) for n in range(refs_per_seq)]
        total = counts[0]
        for c in counts[1:]:
            total = total + c
        if fresh_refs:
            needed = total >= 0
        else:
            needed = (home >= 0) & (home < shards) & (total > 0)
        lane = lax.broadcasted_iota(jnp.int32, (row_count, LANES), 1)

        @pl.when(needed)
        def _():
            tile = jnp.zeros((row_count, LANES), jnp.float32)
            stacked = group * row_count
            key_lane = lax.broadcasted_iota(jnp.int32, (stacked, PAGE), 1)
            for h in range(heads_kv):
                cols = slice(h * HD, (h + 1) * HD)
                q = jnp.concatenate(
                    [
                        query_ref[0, :, (h * group + g) * HD : (h * group + g + 1) * HD]
                        for g in range(group)
                    ],
                    axis=0,
                )
                scores = []
                values = []
                for n in range(refs_per_seq):
                    s = lax.dot_general(
                        q,
                        page_refs[n][0, 0, :, cols],
                        (((1,), (1,)), ((), ())),
                        preferred_element_type=jnp.float32,
                    )
                    scores.append(jnp.where(key_lane < counts[n], s * scale, NO_KEY))
                    values.append(page_refs[n][0, 1, :, cols])
                peak = scores[0]
                for s in scores[1:]:
                    peak = jnp.maximum(peak, s)
                peak = jnp.max(peak, axis=1, keepdims=True)
                if fresh_refs:
                    s = lax.dot_general(
                        q,
                        fresh_refs[0][0, 0, :, cols],
                        (((1,), (1,)), ((), ())),
                        preferred_element_type=jnp.float32,
                    )
                    row = lax.broadcasted_iota(jnp.int32, (stacked, row_count), 0) % row_count
                    col = lax.broadcasted_iota(jnp.int32, (stacked, row_count), 1)
                    live = entry(plan_ref, k, 2 * refs_per_seq) == 1
                    limit = jnp.where(live, row_count, 1)
                    fresh_scores = jnp.where((col <= row) & (col < limit), s * scale, NO_KEY)
                    peak = jnp.maximum(peak, jnp.max(fresh_scores, axis=1, keepdims=True))
                weights = [jnp.exp2(s - peak) for s in scores]
                sums = weights[0]
                for w in weights[1:]:
                    sums = sums + w
                weight_sum = jnp.sum(sums, axis=1, keepdims=True)
                numerator = lax.dot_general(
                    jnp.concatenate([w.astype(jnp.bfloat16) for w in weights], axis=1),
                    jnp.concatenate(values, axis=0),
                    (((1,), (0,)), ((), ())),
                    preferred_element_type=jnp.float32,
                )
                if fresh_refs:
                    w = jnp.exp2(fresh_scores - peak)
                    weight_sum = weight_sum + jnp.sum(w, axis=1, keepdims=True)
                    numerator = numerator + lax.dot_general(
                        w.astype(jnp.bfloat16),
                        fresh_refs[0][1, 0, :, cols],
                        (((1,), (0,)), ((), ())),
                        preferred_element_type=jnp.float32,
                    )
                attended = (numerator / weight_sum).astype(jnp.bfloat16)
                lse = peak + jnp.log2(weight_sum)
                for g in range(group):
                    head = h * group + g
                    rows = slice(g * row_count, (g + 1) * row_count)
                    out_ref[0, :, head * HD : (head + 1) * HD] = attended[rows]
                    mine = (lane == head) | (lane == head + heads) | (lane == head + 2 * heads)
                    tile = jnp.where(mine, lse[rows], tile)
            out_ref[0, :, width:] = lse_block(tile, heads)

        @pl.when(jnp.logical_not(needed))
        def _():
            out_ref[0, :, :width] = jnp.zeros((row_count, width), jnp.bfloat16)
            out_ref[0, :, width:] = lse_block(
                jnp.full((row_count, LANES), NO_KEY, jnp.float32), heads
            )

    page_block = (1, 2, PAGE, part_width)
    in_specs = [pl.BlockSpec((1, row_count, width), lambda k, p: (k, 0, 0))]
    operands = [query]
    for n in range(picks):
        in_specs.append(
            pl.BlockSpec(page_block, lambda k, p, n=n: (entry(p, k, n), 0, 0, p[1]))
        )
        operands.append(pages)
    for n in range(picks, refs_per_seq):
        in_specs.append(pl.BlockSpec(page_block, lambda k, p, n=n: (entry(p, k, n), 0, 0, 0)))
        operands.append(twin_pages)
    if fresh is not None:
        in_specs.append(
            pl.BlockSpec((2, 1, row_count, part_width), lambda k, p: (0, k, 0, 0))
        )
        operands.append(fresh)
    return pl.pallas_call(
        body,
        grid_spec=pltpu.PrefetchScalarGridSpec(
            num_scalar_prefetch=1,
            grid=(count,),
            in_specs=in_specs,
            out_specs=pl.BlockSpec((1, row_count, width + LANES), lambda k, p: (k, 0, 0)),
        ),
        out_shape=jax.ShapeDtypeStruct((count, row_count, width + LANES), jnp.bfloat16),
        name="partial_attention",
        cost_estimate=pl.CostEstimate(
            flops=count * heads * row_count * refs_per_seq * PAGE * HD * 4,
            bytes_accessed=count * row_count * width * 8,
            transcendentals=count * heads * row_count * refs_per_seq * PAGE,
        ),
    )(plan, *operands)


def merge_weights(lses):
    peak = lses[0]
    for lse in lses[1:]:
        peak = jnp.maximum(peak, lse)
    weights = [jnp.exp2(lse - peak) for lse in lses]
    total = weights[0]
    for w in weights[1:]:
        total = total + w
    return [w / total for w in weights], peak + jnp.log2(total)


def merge_pair(plan, mine, incoming, *, chip):
    count, row_count, full = mine.shape
    width = full - LANES
    heads = width // HD

    def body(plan_ref, mine_ref, incoming_ref, out_ref):
        @pl.when(plan_ref[0] == chip)
        def _():
            parts = [mine_ref, incoming_ref]
            lses = [read_lse(r[0, :, width:], heads) for r in parts]
            weights, lse = merge_weights(lses)
            for h in range(heads):
                cols = slice(h * HD, (h + 1) * HD)
                out_ref[0, :, cols] = sum(
                    r[0, :, cols].astype(jnp.float32) * w[:, h : h + 1]
                    for r, w in zip(parts, weights)
                ).astype(jnp.bfloat16)
            out_ref[0, :, width:] = lse_block(spread_lse(lse, heads), heads)

    block = pl.BlockSpec((1, row_count, full), lambda k, p: (k, 0, 0))
    return pl.pallas_call(
        body,
        grid_spec=pltpu.PrefetchScalarGridSpec(
            num_scalar_prefetch=1, grid=(count,), in_specs=[block, block], out_specs=block
        ),
        out_shape=jax.ShapeDtypeStruct(mine.shape, jnp.bfloat16),
        name="merge_pair",
        cost_estimate=pl.CostEstimate(
            flops=count * row_count * width * 8, bytes_accessed=count * row_count * full * 6,
            transcendentals=0,
        ),
    )(plan, mine, incoming)


def merge_final(plan, own, from_right, from_left, *, first, shards, seq_dev, record):
    count, row_count, full = own.shape
    width = full - LANES
    heads = width // HD
    rights = len(from_right)

    def body(plan_ref, own_ref, *rest):
        right_refs = rest[:rights]
        left_refs = rest[rights : rights + len(from_left)]
        out_ref, right_buf, left_buf, sems = rest[rights + len(from_left) :]
        shard = plan_ref[0]
        for s, r in enumerate(right_refs):
            @pl.when(shard == s)
            def _(r=r):
                pltpu.make_async_copy(r, right_buf, sems.at[0]).start()
        for s, r in enumerate(left_refs):
            @pl.when(shard == s + 1)
            def _(r=r):
                pltpu.make_async_copy(r, left_buf, sems.at[1]).start()

        @pl.when(shard < shards - 1)
        def _():
            pltpu.make_async_copy(right_refs[0], right_buf, sems.at[0]).wait()

        @pl.when(shard > 0)
        def _():
            pltpu.make_async_copy(left_refs[0], left_buf, sems.at[1]).wait()

        def one(k, carry):
            empty = jnp.full((row_count, LANES), NO_KEY, jnp.float32)
            right_lse = read_lse(right_buf[k, :, width:], heads)
            left_lse = read_lse(left_buf[k, :, width:], heads)
            right_on = shard < shards - 1
            left_on = shard > 0
            lses = [
                read_lse(own_ref[k, :, width:], heads),
                jnp.where(right_on, right_lse, empty),
                jnp.where(left_on, left_lse, empty),
            ]
            weights, _ = merge_weights(lses)
            row = lax.broadcasted_iota(jnp.int32, (row_count, HD), 0)
            flag = plan_ref[2 + (shard * seq_dev + first + k) * record + record - 1]
            live = row < jnp.where(flag == 1, row_count, 1)
            for h in range(heads):
                cols = slice(h * HD, (h + 1) * HD)
                total = own_ref[k, :, cols].astype(jnp.float32) * weights[0][:, h : h + 1]
                total = total + jnp.where(
                    right_on, right_buf[k, :, cols].astype(jnp.float32), 0.0
                ) * weights[1][:, h : h + 1]
                total = total + jnp.where(
                    left_on, left_buf[k, :, cols].astype(jnp.float32), 0.0
                ) * weights[2][:, h : h + 1]
                out_ref[k, :, cols] = jnp.where(live, total, 0.0).astype(jnp.bfloat16)
            return carry

        lax.fori_loop(0, count, one, 0)

    any_spec = pl.BlockSpec(memory_space=pl.ANY)
    return pl.pallas_call(
        body,
        grid_spec=pltpu.PrefetchScalarGridSpec(
            num_scalar_prefetch=1,
            grid=(1,),
            in_specs=[pl.BlockSpec((count, row_count, full), lambda g, p: (0, 0, 0))]
            + [any_spec] * (rights + len(from_left)),
            out_specs=pl.BlockSpec((count, row_count, width), lambda g, p: (0, 0, 0)),
            scratch_shapes=[
                pltpu.VMEM(own.shape, jnp.bfloat16),
                pltpu.VMEM(own.shape, jnp.bfloat16),
                pltpu.SemaphoreType.DMA((2,)),
            ],
        ),
        out_shape=jax.ShapeDtypeStruct((count, row_count, width), jnp.bfloat16),
        name="merge_final",
    )(plan, own, *from_right, *from_left)


CHUNKS = 2


def queries_travel(queries, new_kv, kv_pages, page_table, cached_len, is_prefill):
    shards = lax.axis_size("seq")
    sub_count = lax.axis_size("sub")
    owners = shards * sub_count
    shard = lax.axis_index("seq")
    core = lax.axis_index("sub")
    seq_dev, row_count, query_width = queries.shape
    pages_dev = kv_pages.shape[0]
    part_width = kv_pages.shape[3] // sub_count
    query_part = query_width // sub_count
    picks = -(-page_table.shape[1] // owners)
    record = 2 * sub_count * picks + 1
    chunk = seq_dev // CHUNKS
    firsts = [n * chunk for n in range(CHUNKS)]
    last = shards - 1

    my_queries = lax.dynamic_slice_in_dim(queries, core * query_part, query_part, 2)
    own_queries = [my_queries[f : f + chunk] for f in firsts]
    twin = lax.dynamic_slice_in_dim(kv_pages, (1 - core) * part_width, part_width, 3)
    twin_pages = lax.ppermute(twin, "sub", [(0, 1), (1, 0)])
    fresh = jnp.transpose(
        lax.dynamic_slice_in_dim(new_kv, core * part_width, part_width, 3), (2, 0, 1, 3)
    )
    plan = page_plan(
        page_table, cached_len, is_prefill, shard, core, pages_dev, sub_count, picks
    )
    common = dict(shards=shards, seq_dev=seq_dev, picks=picks, sub_count=sub_count)

    going_right = [own_queries]
    going_left = [own_queries]
    for h in range(1, shards):
        up = [(a, a + 1) for a in range(h - 1, last)]
        down = [(a, a - 1) for a in range(1, shards - h + 1)]
        rights = []
        lefts = []
        for n in range(CHUNKS):
            rights.append(lax.ppermute(going_right[-1][n], "seq", up))
            lefts.append(lax.ppermute(going_left[-1][n], "seq", down))
        going_right.append(rights)
        going_left.append(lefts)

    def partial(query, offset, n, fresh_part=None):
        return partial_attention(
            plan, query, kv_pages, twin_pages, fresh_part, offset=offset, first=firsts[n], **common
        )

    own = [
        partial(own_queries[n], 0, n, fresh[:, firsts[n] : firsts[n] + chunk])
        for n in range(CHUNKS)
    ]
    outs = []
    from_left_of = {}
    from_right_of = {}
    for h in range(1, shards):
        for n in range(CHUNKS):
            from_left_of[h, n] = partial(going_right[h][n], -h, n)
            from_right_of[h, n] = partial(going_left[h][n], h, n)
    moved_left = {}
    moved_right = {}
    waves = sorted(
        ((last - s) + (last - 1 - l), s, l) for s in range(last) for l in range(s, last)
    )
    for _, s, l in waves:
        for n in range(CHUNKS):
            mine = from_left_of[l + 1 - s, n]
            if l + 1 < last:
                mine = merge_pair(plan, mine, moved_left[s, l + 1, n], chip=l + 1)
            moved_left[s, l, n] = lax.ppermute(mine, "seq", [(l + 1, l)])
            mirror_s, mirror_l = last - s, last - 1 - l
            mine = from_right_of[mirror_s - mirror_l, n]
            if mirror_l > 0:
                mine = merge_pair(plan, mine, moved_right[mirror_s, mirror_l - 1, n], chip=mirror_l)
            moved_right[mirror_s, mirror_l, n] = lax.ppermute(
                mine, "seq", [(mirror_l, mirror_l + 1)]
            )
    for n in range(CHUNKS):
        outs.append(
            merge_final(
                plan,
                own[n],
                [moved_left[s, s, n] for s in range(last)],
                [moved_right[s, s - 1, n] for s in range(1, shards)],
                first=firsts[n],
                shards=shards,
                seq_dev=seq_dev,
                record=record,
            )
        )
    swapped = [lax.ppermute(o, "sub", [(0, 1), (1, 0)]) for o in outs]
    own_half = jnp.concatenate(outs, axis=0)
    other_half = jnp.concatenate(swapped, axis=0)
    first_core = core == 0
    return jnp.concatenate(
        [jnp.where(first_core, own_half, other_half), jnp.where(first_core, other_half, own_half)],
        axis=2,
    )


def per_device(queries, new_kv, kv_pages, page_table, cached_len, is_prefill):
    shards = lax.axis_size("seq")
    sub_count = lax.axis_size("sub")
    heads = queries.shape[2] // sub_count // HD
    spread = page_table.shape[1] >= shards * sub_count and shards > 1 and sub_count == 2
    if spread and 3 * heads <= LANES and queries.shape[0] % CHUNKS == 0:
        return queries_travel(queries, new_kv, kv_pages, page_table, cached_len, is_prefill)
    return pages_travel(queries, new_kv, kv_pages, page_table, cached_len, is_prefill)


def solution(mesh):
    placed = (
        P(("groups", "seq"), None, "head"),
        P(("groups", "seq"), None, None, "head"),
        P(("groups", "seq", "sub"), None, None, "head"),
        P("groups", None),
        P("groups"),
        P("groups"),
    )
    return jax.shard_map(
        per_device,
        mesh=mesh,
        in_specs=placed,
        out_specs=P(("groups", "seq"), None, "head"),
        check_vma=False,
    )
```

```python
import jax
import jax.numpy as jnp
from jax import lax
from jax.experimental import pallas as pl
from jax.experimental.pallas import tpu as pltpu
from jax.sharding import PartitionSpec as P

HD = 128
PAGE = 128


NEG_FILL = -1e30


def partial_softmax(
    query_heads, cache_keys, cache_values, cache_valid, fresh_keys, fresh_values, fresh_valid
):
    score_scale = HD ** (-0.5)
    cache_scores = (
        jnp.einsum("rkgd,nkd->kgrn", query_heads, cache_keys, preferred_element_type=jnp.float32)
        * score_scale
    )
    fresh_scores = (
        jnp.einsum("rkgd,jkd->kgrj", query_heads, fresh_keys, preferred_element_type=jnp.float32)
        * score_scale
    )
    cache_mask = cache_valid[None, None, None, :]
    fresh_mask = fresh_valid[None, None, :, :]
    peak = jnp.maximum(
        jnp.max(jnp.where(cache_mask, cache_scores, NEG_FILL), axis=-1),
        jnp.max(jnp.where(fresh_mask, fresh_scores, NEG_FILL), axis=-1),
    )
    cache_weights = jnp.where(cache_mask, jnp.exp(cache_scores - peak[..., None]), 0.0)
    fresh_weights = jnp.where(fresh_mask, jnp.exp(fresh_scores - peak[..., None]), 0.0)
    weight_sum = jnp.sum(cache_weights, axis=-1) + jnp.sum(fresh_weights, axis=-1)
    numerator = jnp.einsum(
        "kgrn,nkd->kgrd",
        cache_weights.astype(jnp.bfloat16),
        cache_values,
        preferred_element_type=jnp.float32,
    )
    numerator = numerator + jnp.einsum(
        "kgrj,jkd->kgrd",
        fresh_weights.astype(jnp.bfloat16),
        fresh_values,
        preferred_element_type=jnp.float32,
    )
    return (peak, weight_sum, numerator)


def attend_all(
    query_block, fresh_block, received, fetch_index, page_here, lengths, live_rows, causal, fresh_on
):
    kv_width = received.shape[-1]
    heads_kv = kv_width // HD
    row_count = query_block.shape[1]
    group_size = query_block.shape[2] // kv_width
    page_count = fetch_index.shape[1]
    positions = jnp.arange(page_count * PAGE, dtype=jnp.int32)

    def one_sequence(inputs):
        query_rows, fresh_rows, index_row, here_row, length, live_row = inputs
        fetched = jnp.take(received, index_row, axis=0)
        cache_keys = fetched[:, 0].reshape(page_count * PAGE, heads_kv, HD)
        cache_values = fetched[:, 1].reshape(page_count * PAGE, heads_kv, HD)
        page_mask = jnp.broadcast_to(here_row[:, None], (page_count, PAGE)).reshape(
            page_count * PAGE
        )
        cache_valid = page_mask & (positions < length)
        query_heads = query_rows.reshape(row_count, heads_kv, group_size, HD)
        fresh_keys = fresh_rows[:, 0].reshape(row_count, heads_kv, HD)
        fresh_values = fresh_rows[:, 1].reshape(row_count, heads_kv, HD)
        fresh_valid = causal & live_row[:, None] & fresh_on
        return partial_softmax(
            query_heads,
            cache_keys,
            cache_values,
            cache_valid,
            fresh_keys,
            fresh_values,
            fresh_valid,
        )

    return lax.map(
        one_sequence, (query_block, fresh_block, fetch_index, page_here, lengths, live_rows)
    )


def finish(weight_sum, numerator, live_rows):
    unused_rows = 1.0 - live_rows.astype(jnp.float32)
    attended = numerator / (weight_sum + unused_rows[:, None, None, :])[..., None]
    attended = jnp.where(live_rows[:, None, None, :, None], attended, 0.0)
    seq_dev, heads_kv, group_size, row_count, head_dim = attended.shape
    return (
        jnp.transpose(attended, (0, 3, 1, 2, 4))
        .reshape(seq_dev, row_count, heads_kv * group_size * head_dim)
        .astype(jnp.bfloat16)
    )


def pages_travel(queries, new_kv, kv_pages, page_table, cached_len, is_prefill):
    seq_shards = lax.axis_size("seq")
    sub_count = lax.axis_size("sub")
    owners = seq_shards * sub_count
    seq_index = lax.axis_index("seq")
    core_index = lax.axis_index("sub")
    owner_self = seq_index * sub_count + core_index
    seq_dev, row_count, query_width = queries.shape
    pages_dev = kv_pages.shape[0]
    kv_width = kv_pages.shape[3]
    page_count = page_table.shape[1]
    entries = seq_dev * page_count
    capacity = (entries + owners - 1) // owners
    table_rows = page_table.reshape(seq_shards, entries)
    holder = jnp.where(table_rows >= 0, table_rows // pages_dev, -1)
    slot_of = jnp.where(table_rows >= 0, table_rows % pages_dev, 0)
    owned_here = holder == owner_self
    rank_among = jnp.cumsum(owned_here.astype(jnp.int32), axis=1) - 1
    picked = owned_here[:, :, None] & (
        rank_among[:, :, None] == jnp.arange(capacity, dtype=jnp.int32)[None, None, :]
    )
    send_slots = jnp.sum(jnp.where(picked, slot_of[:, :, None], 0), axis=1).reshape(
        seq_shards * capacity
    )
    first_seq = seq_index * seq_dev
    my_table = lax.dynamic_slice_in_dim(page_table, first_seq, seq_dev, 0)
    my_lengths = lax.dynamic_slice_in_dim(cached_len, first_seq, seq_dev, 0)
    my_flags = lax.dynamic_slice_in_dim(is_prefill, first_seq, seq_dev, 0)
    flat_table = my_table.reshape(entries)
    my_holder = jnp.where(flat_table >= 0, flat_table // pages_dev, -1)
    entry_order = jnp.arange(entries, dtype=jnp.int32)
    earlier = (my_holder[:, None] == my_holder[None, :]) & (
        entry_order[None, :] < entry_order[:, None]
    )
    my_rank = jnp.sum(earlier.astype(jnp.int32), axis=1)
    row_ids = jnp.arange(row_count, dtype=jnp.int32)
    live_rows = (my_flags[:, None] == 1) | (row_ids[None, :] == 0)
    causal = row_ids[None, :] <= row_ids[:, None]
    part_width = kv_width // sub_count
    split_pages = kv_pages.reshape(pages_dev, 2, PAGE, sub_count, part_width)
    chosen = jnp.take(split_pages, send_slots, axis=0).reshape(
        seq_shards, capacity, 2, PAGE, sub_count, part_width
    )
    outgoing = jnp.moveaxis(chosen, 4, 1).reshape(owners, capacity, 2, PAGE, part_width)
    received = lax.all_to_all(
        outgoing, ("seq", "sub"), split_axis=0, concat_axis=0, tiled=True
    ).reshape(owners * capacity, 2, PAGE, part_width)
    present = flat_table >= 0
    fetch_index = jnp.where(present, my_holder * capacity + my_rank, 0)
    query_part = query_width // sub_count
    my_queries = lax.dynamic_slice_in_dim(queries, core_index * query_part, query_part, 2)
    my_fresh = lax.dynamic_slice_in_dim(new_kv, core_index * part_width, part_width, 3)
    peak, weight_sum, numerator = attend_all(
        my_queries,
        my_fresh,
        received,
        fetch_index.reshape(seq_dev, page_count),
        present.reshape(seq_dev, page_count),
        my_lengths,
        live_rows,
        causal,
        core_index >= 0,
    )
    own_heads = finish(weight_sum, numerator, live_rows)
    return lax.all_gather(own_heads, "sub", axis=2, tiled=True)


LOG2E = 1.4426950408889634
LANES = 128
NO_KEY = -1e30


def page_plan(page_table, cached_len, is_prefill, shard, core, pages_dev, sub_count, picks):
    seqs, page_count = page_table.shape
    present = page_table >= 0
    owner = jnp.where(present, page_table // pages_dev, -1)
    slot = jnp.where(present, page_table % pages_dev, 0)
    page_ids = jnp.arange(page_count, dtype=jnp.int32)
    keys_here = jnp.clip(cached_len[:, None] - page_ids[None, :] * PAGE, 0, PAGE)
    before = page_ids[None, :] < page_ids[:, None]
    same = owner[:, :, None] == owner[:, None, :]
    rank = jnp.sum((same & before[None]).astype(jnp.int32), axis=2)
    cores = (core + jnp.arange(sub_count, dtype=jnp.int32)) % sub_count
    wanted = shard * sub_count + cores
    picked = (owner[:, None, None, :] == wanted[None, :, None, None]) & (
        rank[:, None, None, :] == jnp.arange(picks, dtype=jnp.int32)[None, None, :, None]
    )
    slots = jnp.sum(jnp.where(picked, slot[:, None, None, :], 0), axis=3)
    counts = jnp.sum(jnp.where(picked, keys_here[:, None, None, :], 0), axis=3)
    rows = jnp.concatenate(
        [
            slots.reshape(seqs, sub_count * picks),
            counts.reshape(seqs, sub_count * picks),
            is_prefill[:, None].astype(jnp.int32),
        ],
        axis=1,
    )
    return jnp.concatenate([jnp.stack([shard, core]).astype(jnp.int32), rows.reshape(-1)])


def lse_block(lse_tile, heads):
    lane = lax.broadcasted_iota(jnp.int32, lse_tile.shape, 1)
    high = lse_tile.astype(jnp.bfloat16)
    rest = lse_tile - high.astype(jnp.float32)
    middle = rest.astype(jnp.bfloat16)
    low = rest - middle.astype(jnp.float32)
    mixed = jnp.where(
        lane < heads,
        high.astype(jnp.float32),
        jnp.where(lane < 2 * heads, middle.astype(jnp.float32), low),
    )
    return mixed.astype(jnp.bfloat16)


def read_lse(block, heads):
    tile = block.astype(jnp.float32)
    return (
        tile
        + pltpu.roll(tile, LANES - heads, 1)
        + pltpu.roll(tile, LANES - 2 * heads, 1)
    )


def spread_lse(lse, heads):
    lane = lax.broadcasted_iota(jnp.int32, lse.shape, 1)
    return jnp.where(
        lane < heads,
        lse,
        jnp.where(lane < 2 * heads, pltpu.roll(lse, heads, 1), pltpu.roll(lse, 2 * heads, 1)),
    )


def work_item(chip, item, shards):
    if 2 * chip >= shards:
        return ("right", item, -item) if item <= chip else ("left", item - chip, item - chip)
    far = shards - 1 - chip
    return ("left", item, item) if item <= far else ("right", item - far, far - item)


def by_chip(shard, values):
    picked = values[0]
    for chip in range(1, len(values)):
        if values[chip] != values[chip - 1]:
            picked = jnp.where(shard >= chip, values[chip], picked)
    return picked


def partial_attention(
    plan, sources, choice, homes, pages, twin_pages, fresh, after, *, first, seq_dev, picks, sub_count
):
    count, row_count, width = sources[0].shape
    part_width = twin_pages.shape[3]
    heads_kv = part_width // HD
    heads = width // HD
    group = heads // heads_kv
    refs_per_seq = sub_count * picks
    record = 2 * refs_per_seq + 1
    scale = LOG2E * HD ** (-0.5)
    few = min(row_count, 16)

    def entry(plan_ref, k, column):
        home = by_chip(plan_ref[0], homes)
        return plan_ref[2 + (home * seq_dev + first + k) * record + column]

    def body(plan_ref, *rest):
        query_refs = rest[: len(sources)]
        page_refs = rest[len(sources) : len(sources) + refs_per_seq]
        fresh_ref = rest[len(sources) + refs_per_seq] if fresh is not None else None
        out_ref, query_buf = rest[-2:]
        k = pl.program_id(0)
        shard = plan_ref[0]
        counts = [entry(plan_ref, k, refs_per_seq + n) for n in range(refs_per_seq)]
        flag = entry(plan_ref, k, 2 * refs_per_seq)
        if len(sources) == 1:
            query_ref = query_refs[0]
        else:
            query_ref = query_buf
            for n in range(len(sources)):
                chips = [chip for chip, c in enumerate(choice) if c == n]
                chosen = shard == chips[0]
                for chip in chips[1:]:
                    chosen = chosen | (shard == chip)

                @pl.when(chosen)
                def _(n=n):
                    query_buf[...] = query_refs[n][...]

        def attend(rows, live_rows):
            lane = lax.broadcasted_iota(jnp.int32, (rows, LANES), 1)
            tile = jnp.zeros((rows, LANES), jnp.float32)
            per_block = max(1, min(group, BLOCK_ROWS // rows))
            stacked = per_block * rows
            key_lane = lax.broadcasted_iota(jnp.int32, (stacked, PAGE), 1)
            for h in range(heads_kv):
                cols = slice(h * HD, (h + 1) * HD)
                keys = jnp.concatenate([r[0, 0, :, cols] for r in page_refs], axis=0)
                values = jnp.concatenate([r[0, 1, :, cols] for r in page_refs], axis=0)
                for g0 in range(0, group, per_block):
                    base = h * group + g0
                    q = jnp.concatenate(
                        [
                            query_ref[0, :rows, (base + g) * HD : (base + g + 1) * HD]
                            for g in range(per_block)
                        ],
                        axis=0,
                    )
                    s = lax.dot_general(
                        q, keys, (((1,), (1,)), ((), ())), preferred_element_type=jnp.float32
                    )
                    scores = [
                        jnp.where(
                            key_lane < counts[n], s[:, n * PAGE : (n + 1) * PAGE] * scale, NO_KEY
                        )
                        for n in range(refs_per_seq)
                    ]
                    peak = scores[0]
                    for x in scores[1:]:
                        peak = jnp.maximum(peak, x)
                    peak = jnp.max(peak, axis=1, keepdims=True)
                    if fresh is not None:
                        s = lax.dot_general(
                            q,
                            fresh_ref[0, 0, :, cols],
                            (((1,), (1,)), ((), ())),
                            preferred_element_type=jnp.float32,
                        )
                        row = lax.broadcasted_iota(jnp.int32, (stacked, row_count), 0) % rows
                        col = lax.broadcasted_iota(jnp.int32, (stacked, row_count), 1)
                        new_scores = jnp.where(
                            (col <= row) & (col < live_rows), s * scale, NO_KEY
                        )
                        peak = jnp.maximum(peak, jnp.max(new_scores, axis=1, keepdims=True))
                    weights = [jnp.exp2(x - peak) for x in scores]
                    sums = weights[0]
                    for w in weights[1:]:
                        sums = sums + w
                    weight_sum = jnp.sum(sums, axis=1, keepdims=True)
                    numerator = lax.dot_general(
                        jnp.concatenate([w.astype(jnp.bfloat16) for w in weights], axis=1),
                        values,
                        (((1,), (0,)), ((), ())),
                        preferred_element_type=jnp.float32,
                    )
                    if fresh is not None:
                        w = jnp.exp2(new_scores - peak)
                        weight_sum = weight_sum + jnp.sum(w, axis=1, keepdims=True)
                        numerator = numerator + lax.dot_general(
                            w.astype(jnp.bfloat16),
                            fresh_ref[1, 0, :, cols],
                            (((1,), (0,)), ((), ())),
                            preferred_element_type=jnp.float32,
                        )
                    attended = (numerator / weight_sum).astype(jnp.bfloat16)
                    lse = peak + jnp.log2(weight_sum)
                    for g in range(per_block):
                        head = base + g
                        part = slice(g * rows, (g + 1) * rows)
                        out_ref[0, :rows, head * HD : (head + 1) * HD] = attended[part]
                        mine = (lane == head) | (lane == head + heads) | (lane == head + 2 * heads)
                        tile = jnp.where(mine, lse[part], tile)
            out_ref[0, :rows, width:] = lse_block(tile, heads)

        @pl.when(flag == 1)
        def _():
            attend(row_count, row_count)

        @pl.when(flag != 1)
        def _():
            attend(few, 1)
            if few < row_count:
                out_ref[0, few:, :] = jnp.zeros((row_count - few, width + LANES), jnp.bfloat16)

    page_block = (1, 2, PAGE, part_width)
    in_specs = [pl.BlockSpec((1, row_count, width), lambda k, p: (k, 0, 0)) for _ in sources]
    operands = list(sources)
    for n in range(picks):
        in_specs.append(
            pl.BlockSpec(page_block, lambda k, p, n=n: (entry(p, k, n), 0, 0, p[1]))
        )
        operands.append(pages)
    for n in range(picks, refs_per_seq):
        in_specs.append(pl.BlockSpec(page_block, lambda k, p, n=n: (entry(p, k, n), 0, 0, 0)))
        operands.append(twin_pages)
    if fresh is not None:
        in_specs.append(
            pl.BlockSpec((2, 1, row_count, part_width), lambda k, p: (0, k, 0, 0))
        )
        operands.append(fresh)
    for x in after:
        in_specs.append(pl.BlockSpec(memory_space=pl.ANY))
        operands.append(x)
    return pl.pallas_call(
        body,
        grid_spec=pltpu.PrefetchScalarGridSpec(
            num_scalar_prefetch=1,
            grid=(count,),
            in_specs=in_specs,
            out_specs=pl.BlockSpec((1, row_count, width + LANES), lambda k, p: (k, 0, 0)),
            scratch_shapes=[pltpu.VMEM((1, row_count, width), jnp.bfloat16)],
        ),
        out_shape=jax.ShapeDtypeStruct((count, row_count, width + LANES), jnp.bfloat16),
        name="partial_attention",
        cost_estimate=pl.CostEstimate(
            flops=count * heads * row_count * refs_per_seq * PAGE * HD * 4,
            bytes_accessed=count * row_count * width * 8,
            transcendentals=count * heads * row_count * refs_per_seq * PAGE,
        ),
    )(plan, *operands)


def merge_weights(lses):
    peak = lses[0]
    for lse in lses[1:]:
        peak = jnp.maximum(peak, lse)
    weights = [jnp.exp2(lse - peak) for lse in lses]
    total = weights[0]
    for w in weights[1:]:
        total = total + w
    return [w / total for w in weights], peak + jnp.log2(total)


def merge_pair(plan, mine, incoming, *, chips):
    count, row_count, full = mine.shape
    width = full - LANES
    heads = width // HD

    def body(plan_ref, mine_hbm, incoming_hbm, out_ref, mine_ref, incoming_ref, sems):
        here = plan_ref[0] == chips[0]
        for chip in chips[1:]:
            here = here | (plan_ref[0] == chip)

        @pl.when(here)
        def _():
            copies = [
                pltpu.make_async_copy(mine_hbm, mine_ref, sems.at[0]),
                pltpu.make_async_copy(incoming_hbm, incoming_ref, sems.at[1]),
            ]
            for c in copies:
                c.start()
            for c in copies:
                c.wait()
            parts = [mine_ref, incoming_ref]
            for k in range(count):
                weights, lse = merge_weights([read_lse(r[k, :, width:], heads) for r in parts])
                for h in range(heads):
                    cols = slice(h * HD, (h + 1) * HD)
                    out_ref[k, :, cols] = sum(
                        r[k, :, cols].astype(jnp.float32) * w[:, h : h + 1]
                        for r, w in zip(parts, weights)
                    ).astype(jnp.bfloat16)
                out_ref[k, :, width:] = lse_block(spread_lse(lse, heads), heads)

    any_spec = pl.BlockSpec(memory_space=pl.ANY)
    return pl.pallas_call(
        body,
        grid_spec=pltpu.PrefetchScalarGridSpec(
            num_scalar_prefetch=1,
            grid=(1,),
            in_specs=[any_spec, any_spec],
            out_specs=pl.BlockSpec(mine.shape, lambda g, p: (0, 0, 0)),
            scratch_shapes=[
                pltpu.VMEM(mine.shape, jnp.bfloat16),
                pltpu.VMEM(mine.shape, jnp.bfloat16),
                pltpu.SemaphoreType.DMA((2,)),
            ],
        ),
        out_shape=jax.ShapeDtypeStruct(mine.shape, jnp.bfloat16),
        name="merge_pair",
    )(plan, mine, incoming)


def merge_final(plan, own, arrived, *, first, shards, seq_dev, record):
    count, row_count, full = own.shape
    width = full - LANES
    heads = width // HD
    last = shards - 1

    def body(plan_ref, own_ref, *rest):
        arrived_refs = rest[:last]
        out_ref, right_buf, left_buf, sems = rest[last:]
        shard = plan_ref[0]
        for s, r in enumerate(arrived_refs):
            @pl.when(shard == s)
            def _(r=r):
                pltpu.make_async_copy(r, right_buf, sems.at[0]).start()

            @pl.when(shard == last - s)
            def _(r=r):
                pltpu.make_async_copy(r, left_buf, sems.at[1]).start()

        @pl.when(shard < shards - 1)
        def _():
            pltpu.make_async_copy(arrived_refs[0], right_buf, sems.at[0]).wait()

        @pl.when(shard > 0)
        def _():
            pltpu.make_async_copy(arrived_refs[0], left_buf, sems.at[1]).wait()

        def one(k, carry):
            empty = jnp.full((row_count, LANES), NO_KEY, jnp.float32)
            right_lse = read_lse(right_buf[k, :, width:], heads)
            left_lse = read_lse(left_buf[k, :, width:], heads)
            right_on = shard < shards - 1
            left_on = shard > 0
            lses = [
                read_lse(own_ref[k, :, width:], heads),
                jnp.where(right_on, right_lse, empty),
                jnp.where(left_on, left_lse, empty),
            ]
            weights, _ = merge_weights(lses)
            row = lax.broadcasted_iota(jnp.int32, (row_count, HD), 0)
            flag = plan_ref[2 + (shard * seq_dev + first + k) * record + record - 1]
            live = row < jnp.where(flag == 1, row_count, 1)
            for h in range(heads):
                cols = slice(h * HD, (h + 1) * HD)
                total = own_ref[k, :, cols].astype(jnp.float32) * weights[0][:, h : h + 1]
                total = total + jnp.where(
                    right_on, right_buf[k, :, cols].astype(jnp.float32), 0.0
                ) * weights[1][:, h : h + 1]
                total = total + jnp.where(
                    left_on, left_buf[k, :, cols].astype(jnp.float32), 0.0
                ) * weights[2][:, h : h + 1]
                out_ref[k, :, cols] = jnp.where(live, total, 0.0).astype(jnp.bfloat16)
            return carry

        lax.fori_loop(0, count, one, 0)

    any_spec = pl.BlockSpec(memory_space=pl.ANY)
    return pl.pallas_call(
        body,
        grid_spec=pltpu.PrefetchScalarGridSpec(
            num_scalar_prefetch=1,
            grid=(1,),
            in_specs=[pl.BlockSpec((count, row_count, full), lambda g, p: (0, 0, 0))]
            + [any_spec] * last,
            out_specs=pl.BlockSpec((count, row_count, width), lambda g, p: (0, 0, 0)),
            scratch_shapes=[
                pltpu.VMEM(own.shape, jnp.bfloat16),
                pltpu.VMEM(own.shape, jnp.bfloat16),
                pltpu.SemaphoreType.DMA((2,)),
            ],
        ),
        out_shape=jax.ShapeDtypeStruct((count, row_count, width), jnp.bfloat16),
        name="merge_final",
    )(plan, own, *arrived)


CHUNKS = 2
BLOCK_ROWS = 512


def queries_travel(queries, new_kv, kv_pages, page_table, cached_len, is_prefill):
    shards = lax.axis_size("seq")
    sub_count = lax.axis_size("sub")
    owners = shards * sub_count
    shard = lax.axis_index("seq")
    core = lax.axis_index("sub")
    seq_dev, row_count, query_width = queries.shape
    pages_dev = kv_pages.shape[0]
    part_width = kv_pages.shape[3] // sub_count
    query_part = query_width // sub_count
    picks = -(-page_table.shape[1] // owners)
    record = 2 * sub_count * picks + 1
    chunk = seq_dev // CHUNKS
    firsts = [n * chunk for n in range(CHUNKS)]
    last = shards - 1

    my_queries = lax.dynamic_slice_in_dim(queries, core * query_part, query_part, 2)
    my_queries, later_pages = lax.optimization_barrier((my_queries, kv_pages))
    own_queries = [my_queries[f : f + chunk] for f in firsts]
    plan = page_plan(
        page_table, cached_len, is_prefill, shard, core, pages_dev, sub_count, picks
    )

    twin = lax.dynamic_slice_in_dim(later_pages, (1 - core) * part_width, part_width, 3)
    twin_pages = lax.ppermute(twin, "sub", [(0, 1), (1, 0)])
    fresh = jnp.transpose(
        lax.dynamic_slice_in_dim(new_kv, core * part_width, part_width, 3), (2, 0, 1, 3)
    )

    def partial(n, sources, choice, homes, fresh_part=None, after=()):
        return partial_attention(
            plan,
            sources,
            choice,
            homes,
            kv_pages,
            twin_pages,
            fresh_part,
            after,
            first=firsts[n],
            seq_dev=seq_dev,
            picks=picks,
            sub_count=sub_count,
        )

    own = [
        partial(
            n,
            [own_queries[n]],
            [0] * shards,
            list(range(shards)),
            fresh[:, firsts[n] : firsts[n] + chunk],
        )
        for n in range(CHUNKS)
    ]
    hops = {"right": [own_queries], "left": [own_queries]}
    work = {}
    previous = tuple(own)

    def attend(item, previous):
        items = [work_item(chip, item, shards) for chip in range(shards)]
        kinds = sorted({(way, h) for way, h, _ in items})
        choice = [kinds.index((way, h)) for way, h, _ in items]
        homes = [chip + offset for chip, (_, _, offset) in enumerate(items)]
        for n in range(CHUNKS):
            work[item, n] = partial(
                n, [hops[way][h][n] for way, h in kinds], choice, homes, after=previous
            )
            previous = (work[item, n],)
        return previous

    for h in range(1, shards):
        up = [(a, a + 1) for a in range(h - 1, last)]
        down = [(a, a - 1) for a in range(1, shards - h + 1)]
        moved = {"right": [], "left": []}
        for n in range(CHUNKS):
            for way, pairs in (("right", up), ("left", down)):
                leaving = hops[way][-1][n]
                if h > 1:
                    gate = own[n] if h == 2 else work[h - 2, n]
                    leaving, _ = lax.optimization_barrier((leaving, gate))
                moved[way].append(lax.ppermute(leaving, "seq", pairs))
        for way in hops:
            hops[way].append(moved[way])
        previous = attend(h, previous)

    moved = {}
    waves = sorted(
        ((last - s) + (last - 1 - l), s, l) for s in range(last) for l in range(s, last)
    )
    for _, s, l in waves:
        sender = l + 1
        mirror = last - sender
        way = ("right", sender - s)
        item = next(w for w in range(1, shards) if work_item(sender, w, shards)[:2] == way)
        pairs = [(sender, sender - 1), (mirror, mirror + 1)]
        for n in range(CHUNKS):
            mine = work[item, n]
            if sender < last:
                mine = merge_pair(plan, mine, moved[s, l + 1, n], chips=(sender, mirror))
            moved[s, l, n] = lax.ppermute(mine, "seq", pairs)
    outs = [
        merge_final(
            plan,
            own[n],
            [moved[s, s, n] for s in range(last)],
            first=firsts[n],
            shards=shards,
            seq_dev=seq_dev,
            record=record,
        )
        for n in range(CHUNKS)
    ]
    swapped = [lax.ppermute(o, "sub", [(0, 1), (1, 0)]) for o in outs]
    own_half = jnp.concatenate(outs, axis=0)
    other_half = jnp.concatenate(swapped, axis=0)
    first_core = core == 0
    return jnp.concatenate(
        [jnp.where(first_core, own_half, other_half), jnp.where(first_core, other_half, own_half)],
        axis=2,
    )


def per_device(queries, new_kv, kv_pages, page_table, cached_len, is_prefill):
    shards = lax.axis_size("seq")
    sub_count = lax.axis_size("sub")
    heads = queries.shape[2] // sub_count // HD
    spread = page_table.shape[1] >= shards * sub_count and shards % 2 == 0 and sub_count == 2
    if spread and 3 * heads <= LANES and queries.shape[0] % CHUNKS == 0:
        return queries_travel(queries, new_kv, kv_pages, page_table, cached_len, is_prefill)
    return pages_travel(queries, new_kv, kv_pages, page_table, cached_len, is_prefill)


def solution(mesh):
    placed = (
        P(("groups", "seq"), None, "head"),
        P(("groups", "seq"), None, None, "head"),
        P(("groups", "seq", "sub"), None, None, "head"),
        P("groups", None),
        P("groups"),
        P("groups"),
    )
    return jax.shard_map(
        per_device,
        mesh=mesh,
        in_specs=placed,
        out_specs=P(("groups", "seq"), None, "head"),
        check_vma=False,
    )
```

```python
import jax
import jax.numpy as jnp
from jax import lax
from jax.experimental import pallas as pl
from jax.experimental.pallas import tpu as pltpu
from jax.sharding import PartitionSpec as P


HD = 128
PAGE = 128


NEG_FILL = -1e30


def partial_softmax(
    query_heads, cache_keys, cache_values, cache_valid, fresh_keys, fresh_values, fresh_valid
):
    score_scale = HD ** (-0.5)
    cache_scores = (
        jnp.einsum("rkgd,nkd->kgrn", query_heads, cache_keys, preferred_element_type=jnp.float32)
        * score_scale
    )
    fresh_scores = (
        jnp.einsum("rkgd,jkd->kgrj", query_heads, fresh_keys, preferred_element_type=jnp.float32)
        * score_scale
    )
    cache_mask = cache_valid[None, None, None, :]
    fresh_mask = fresh_valid[None, None, :, :]
    peak = jnp.maximum(
        jnp.max(jnp.where(cache_mask, cache_scores, NEG_FILL), axis=-1),
        jnp.max(jnp.where(fresh_mask, fresh_scores, NEG_FILL), axis=-1),
    )
    cache_weights = jnp.where(cache_mask, jnp.exp(cache_scores - peak[..., None]), 0.0)
    fresh_weights = jnp.where(fresh_mask, jnp.exp(fresh_scores - peak[..., None]), 0.0)
    weight_sum = jnp.sum(cache_weights, axis=-1) + jnp.sum(fresh_weights, axis=-1)
    numerator = jnp.einsum(
        "kgrn,nkd->kgrd",
        cache_weights.astype(jnp.bfloat16),
        cache_values,
        preferred_element_type=jnp.float32,
    )
    numerator = numerator + jnp.einsum(
        "kgrj,jkd->kgrd",
        fresh_weights.astype(jnp.bfloat16),
        fresh_values,
        preferred_element_type=jnp.float32,
    )
    return (peak, weight_sum, numerator)


def attend_all(
    query_block, fresh_block, received, fetch_index, page_here, lengths, live_rows, causal, fresh_on
):
    kv_width = received.shape[-1]
    heads_kv = kv_width // HD
    row_count = query_block.shape[1]
    group_size = query_block.shape[2] // kv_width
    page_count = fetch_index.shape[1]
    positions = jnp.arange(page_count * PAGE, dtype=jnp.int32)

    def one_sequence(inputs):
        query_rows, fresh_rows, index_row, here_row, length, live_row = inputs
        fetched = jnp.take(received, index_row, axis=0)
        cache_keys = fetched[:, 0].reshape(page_count * PAGE, heads_kv, HD)
        cache_values = fetched[:, 1].reshape(page_count * PAGE, heads_kv, HD)
        page_mask = jnp.broadcast_to(here_row[:, None], (page_count, PAGE)).reshape(
            page_count * PAGE
        )
        cache_valid = page_mask & (positions < length)
        query_heads = query_rows.reshape(row_count, heads_kv, group_size, HD)
        fresh_keys = fresh_rows[:, 0].reshape(row_count, heads_kv, HD)
        fresh_values = fresh_rows[:, 1].reshape(row_count, heads_kv, HD)
        fresh_valid = causal & live_row[:, None] & fresh_on
        return partial_softmax(
            query_heads,
            cache_keys,
            cache_values,
            cache_valid,
            fresh_keys,
            fresh_values,
            fresh_valid,
        )

    return lax.map(
        one_sequence, (query_block, fresh_block, fetch_index, page_here, lengths, live_rows)
    )


def finish(weight_sum, numerator, live_rows):
    unused_rows = 1.0 - live_rows.astype(jnp.float32)
    attended = numerator / (weight_sum + unused_rows[:, None, None, :])[..., None]
    attended = jnp.where(live_rows[:, None, None, :, None], attended, 0.0)
    seq_dev, heads_kv, group_size, row_count, head_dim = attended.shape
    return (
        jnp.transpose(attended, (0, 3, 1, 2, 4))
        .reshape(seq_dev, row_count, heads_kv * group_size * head_dim)
        .astype(jnp.bfloat16)
    )


def pages_travel(queries, new_kv, kv_pages, page_table, cached_len, is_prefill):
    seq_shards = lax.axis_size("seq")
    sub_count = lax.axis_size("sub")
    owners = seq_shards * sub_count
    seq_index = lax.axis_index("seq")
    core_index = lax.axis_index("sub")
    owner_self = seq_index * sub_count + core_index
    seq_dev, row_count, query_width = queries.shape
    pages_dev = kv_pages.shape[0]
    kv_width = kv_pages.shape[3]
    page_count = page_table.shape[1]
    entries = seq_dev * page_count
    capacity = (entries + owners - 1) // owners
    table_rows = page_table.reshape(seq_shards, entries)
    holder = jnp.where(table_rows >= 0, table_rows // pages_dev, -1)
    slot_of = jnp.where(table_rows >= 0, table_rows % pages_dev, 0)
    owned_here = holder == owner_self
    rank_among = jnp.cumsum(owned_here.astype(jnp.int32), axis=1) - 1
    picked = owned_here[:, :, None] & (
        rank_among[:, :, None] == jnp.arange(capacity, dtype=jnp.int32)[None, None, :]
    )
    send_slots = jnp.sum(jnp.where(picked, slot_of[:, :, None], 0), axis=1).reshape(
        seq_shards * capacity
    )
    first_seq = seq_index * seq_dev
    my_table = lax.dynamic_slice_in_dim(page_table, first_seq, seq_dev, 0)
    my_lengths = lax.dynamic_slice_in_dim(cached_len, first_seq, seq_dev, 0)
    my_flags = lax.dynamic_slice_in_dim(is_prefill, first_seq, seq_dev, 0)
    flat_table = my_table.reshape(entries)
    my_holder = jnp.where(flat_table >= 0, flat_table // pages_dev, -1)
    entry_order = jnp.arange(entries, dtype=jnp.int32)
    earlier = (my_holder[:, None] == my_holder[None, :]) & (
        entry_order[None, :] < entry_order[:, None]
    )
    my_rank = jnp.sum(earlier.astype(jnp.int32), axis=1)
    row_ids = jnp.arange(row_count, dtype=jnp.int32)
    live_rows = (my_flags[:, None] == 1) | (row_ids[None, :] == 0)
    causal = row_ids[None, :] <= row_ids[:, None]
    part_width = kv_width // sub_count
    split_pages = kv_pages.reshape(pages_dev, 2, PAGE, sub_count, part_width)
    chosen = jnp.take(split_pages, send_slots, axis=0).reshape(
        seq_shards, capacity, 2, PAGE, sub_count, part_width
    )
    outgoing = jnp.moveaxis(chosen, 4, 1).reshape(owners, capacity, 2, PAGE, part_width)
    received = lax.all_to_all(
        outgoing, ("seq", "sub"), split_axis=0, concat_axis=0, tiled=True
    ).reshape(owners * capacity, 2, PAGE, part_width)
    present = flat_table >= 0
    fetch_index = jnp.where(present, my_holder * capacity + my_rank, 0)
    query_part = query_width // sub_count
    my_queries = lax.dynamic_slice_in_dim(queries, core_index * query_part, query_part, 2)
    my_fresh = lax.dynamic_slice_in_dim(new_kv, core_index * part_width, part_width, 3)
    _, weight_sum, numerator = attend_all(
        my_queries,
        my_fresh,
        received,
        fetch_index.reshape(seq_dev, page_count),
        present.reshape(seq_dev, page_count),
        my_lengths,
        live_rows,
        causal,
        core_index >= 0,
    )
    own_heads = finish(weight_sum, numerator, live_rows)
    return lax.all_gather(own_heads, "sub", axis=2, tiled=True)


LOG2E = 1.4426950408889634
LANES = 128
NO_KEY = -1e30


def page_plan(page_table, cached_len, is_prefill, shard, core, pages_dev, sub_count, picks):
    seqs, page_count = page_table.shape
    present = page_table >= 0
    owner = jnp.where(present, page_table // pages_dev, -1)
    slot = jnp.where(present, page_table % pages_dev, 0)
    page_ids = jnp.arange(page_count, dtype=jnp.int32)
    keys_here = jnp.clip(cached_len[:, None] - page_ids[None, :] * PAGE, 0, PAGE)
    before = page_ids[None, :] < page_ids[:, None]
    same = owner[:, :, None] == owner[:, None, :]
    rank = jnp.sum((same & before[None]).astype(jnp.int32), axis=2)
    cores = (core + jnp.arange(sub_count, dtype=jnp.int32)) % sub_count
    wanted = shard * sub_count + cores
    picked = (owner[:, None, None, :] == wanted[None, :, None, None]) & (
        rank[:, None, None, :] == jnp.arange(picks, dtype=jnp.int32)[None, None, :, None]
    )
    slots = jnp.sum(jnp.where(picked, slot[:, None, None, :], 0), axis=3)
    counts = jnp.sum(jnp.where(picked, keys_here[:, None, None, :], 0), axis=3)
    rows = jnp.concatenate(
        [
            slots.reshape(seqs, sub_count * picks),
            counts.reshape(seqs, sub_count * picks),
            is_prefill[:, None].astype(jnp.int32),
        ],
        axis=1,
    )
    return jnp.concatenate([jnp.stack([shard, core]).astype(jnp.int32), rows.reshape(-1)])


def lse_block(lse_tile, heads):
    lane = lax.broadcasted_iota(jnp.int32, lse_tile.shape, 1)
    high = lse_tile.astype(jnp.bfloat16)
    rest = lse_tile - high.astype(jnp.float32)
    middle = rest.astype(jnp.bfloat16)
    low = rest - middle.astype(jnp.float32)
    mixed = jnp.where(
        lane < heads,
        high.astype(jnp.float32),
        jnp.where(lane < 2 * heads, middle.astype(jnp.float32), low),
    )
    return mixed.astype(jnp.bfloat16)


def read_lse(block, heads):
    tile = block.astype(jnp.float32)
    return (
        tile
        + pltpu.roll(tile, LANES - heads, 1)
        + pltpu.roll(tile, LANES - 2 * heads, 1)
    )


def spread_lse(lse, heads):
    lane = lax.broadcasted_iota(jnp.int32, lse.shape, 1)
    return jnp.where(
        lane < heads,
        lse,
        jnp.where(lane < 2 * heads, pltpu.roll(lse, heads, 1), pltpu.roll(lse, 2 * heads, 1)),
    )


def one_of(shard, table, value):
    found = None
    for chip, entry in enumerate(table):
        if entry == value:
            here = shard == chip
            found = here if found is None else found | here
    return found


def by_chip(shard, values):
    picked = values[0]
    for chip in range(1, len(values)):
        if values[chip] != values[chip - 1]:
            picked = jnp.where(shard >= chip, values[chip], picked)
    return picked


def partial_attention(
    plan, sources, choice, homes, pages, twin_pages, fresh, relays, *, count, width, first, seq_dev,
    picks, sub_count
):
    row_count = sources[0].shape[1]
    part_width = twin_pages.shape[3]
    heads_kv = part_width // HD
    heads = width // HD
    group = heads // heads_kv
    refs_per_seq = sub_count * picks
    record = 2 * refs_per_seq + 1
    scale = LOG2E * HD ** (-0.5)
    few = min(row_count, 16)

    def entry(plan_ref, k, column):
        home = by_chip(plan_ref[0], homes)
        return plan_ref[2 + (home * seq_dev + first + k) * record + column]

    def body(plan_ref, *rest):
        query_refs = rest[: len(sources)]
        page_refs = rest[len(sources) : len(sources) + refs_per_seq]
        fresh_ref = rest[len(sources) + refs_per_seq] if fresh is not None else None
        query_buf = rest[-1]
        out_ref = rest[-2 - len(relays)]
        relay_refs = rest[-1 - len(relays) : -1]
        k = pl.program_id(0)
        shard = plan_ref[0]
        counts = [entry(plan_ref, k, refs_per_seq + n) for n in range(refs_per_seq)]
        flag = entry(plan_ref, k, 2 * refs_per_seq)
        if len(sources) == 1:
            query_ref = query_refs[0]
        else:
            query_ref = query_buf
            for n in range(len(sources)):
                @pl.when(one_of(shard, choice, n))
                def _(n=n):
                    query_buf[...] = query_refs[n][...]

        for relay, relay_ref in zip(relays, relay_refs):
            for n in range(len(sources)):
                if n in relay:
                    @pl.when(one_of(shard, relay, n))
                    def _(n=n, relay_ref=relay_ref):
                        relay_ref[0, :, :width] = query_refs[n][0]

        def attend(rows, live_rows):
            lane = lax.broadcasted_iota(jnp.int32, (rows, LANES), 1)
            tile = jnp.zeros((rows, LANES), jnp.float32)
            per_block = max(1, min(group, BLOCK_ROWS // rows))
            stacked = per_block * rows
            key_lane = lax.broadcasted_iota(jnp.int32, (stacked, PAGE), 1)
            for h in range(heads_kv):
                cols = slice(h * HD, (h + 1) * HD)
                keys = jnp.concatenate([r[0, 0, :, cols] for r in page_refs], axis=0)
                values = jnp.concatenate([r[0, 1, :, cols] for r in page_refs], axis=0)
                for g0 in range(0, group, per_block):
                    base = h * group + g0
                    q = jnp.concatenate(
                        [
                            query_ref[0, :rows, (base + g) * HD : (base + g + 1) * HD]
                            for g in range(per_block)
                        ],
                        axis=0,
                    )
                    s = lax.dot_general(
                        q, keys, (((1,), (1,)), ((), ())), preferred_element_type=jnp.float32
                    )
                    scores = [
                        jnp.where(
                            key_lane < counts[n], s[:, n * PAGE : (n + 1) * PAGE] * scale, NO_KEY
                        )
                        for n in range(refs_per_seq)
                    ]
                    peak = scores[0]
                    for x in scores[1:]:
                        peak = jnp.maximum(peak, x)
                    peak = jnp.max(peak, axis=1, keepdims=True)
                    if fresh is not None:
                        s = lax.dot_general(
                            q,
                            fresh_ref[0, 0, :, cols],
                            (((1,), (1,)), ((), ())),
                            preferred_element_type=jnp.float32,
                        )
                        row = lax.broadcasted_iota(jnp.int32, (stacked, row_count), 0) % rows
                        col = lax.broadcasted_iota(jnp.int32, (stacked, row_count), 1)
                        new_scores = jnp.where(
                            (col <= row) & (col < live_rows), s * scale, NO_KEY
                        )
                        peak = jnp.maximum(peak, jnp.max(new_scores, axis=1, keepdims=True))
                    weights = [jnp.exp2(x - peak) for x in scores]
                    sums = weights[0]
                    for w in weights[1:]:
                        sums = sums + w
                    weight_sum = jnp.sum(sums, axis=1, keepdims=True)
                    numerator = lax.dot_general(
                        jnp.concatenate([w.astype(jnp.bfloat16) for w in weights], axis=1),
                        values,
                        (((1,), (0,)), ((), ())),
                        preferred_element_type=jnp.float32,
                    )
                    if fresh is not None:
                        w = jnp.exp2(new_scores - peak)
                        weight_sum = weight_sum + jnp.sum(w, axis=1, keepdims=True)
                        numerator = numerator + lax.dot_general(
                            w.astype(jnp.bfloat16),
                            fresh_ref[1, 0, :, cols],
                            (((1,), (0,)), ((), ())),
                            preferred_element_type=jnp.float32,
                        )
                    attended = (numerator / weight_sum).astype(jnp.bfloat16)
                    lse = peak + jnp.log2(weight_sum)
                    for g in range(per_block):
                        head = base + g
                        part = slice(g * rows, (g + 1) * rows)
                        out_ref[0, :rows, head * HD : (head + 1) * HD] = attended[part]
                        mine = (lane == head) | (lane == head + heads) | (lane == head + 2 * heads)
                        tile = jnp.where(mine, lse[part], tile)
            out_ref[0, :rows, width:] = lse_block(tile, heads)

        @pl.when(flag == 1)
        def _():
            attend(row_count, row_count)

        @pl.when(flag != 1)
        def _():
            attend(few, 1)
            if few < row_count:
                out_ref[0, few:, :] = jnp.zeros((row_count - few, width + LANES), jnp.bfloat16)

        for relay, relay_ref in zip(relays, relay_refs):
            @pl.when(one_of(shard, relay, -1))
            def _(relay_ref=relay_ref):
                relay_ref[...] = out_ref[...]

    page_block = (1, 2, PAGE, part_width)
    if fresh is None:
        in_specs = [pl.BlockSpec((1, row_count, width), lambda k, p: (k, 0, 0)) for _ in sources]
    else:
        in_specs = [pl.BlockSpec((1, row_count, width), lambda k, p: (k, 0, p[1]))]
    operands = list(sources)
    for n in range(picks):
        in_specs.append(
            pl.BlockSpec(page_block, lambda k, p, n=n: (entry(p, k, n), 0, 0, p[1]))
        )
        operands.append(pages)
    for n in range(picks, refs_per_seq):
        in_specs.append(pl.BlockSpec(page_block, lambda k, p, n=n: (entry(p, k, n), 0, 0, 0)))
        operands.append(twin_pages)
    if fresh is not None:
        in_specs.append(
            pl.BlockSpec((2, 1, row_count, part_width), lambda k, p: (0, k, 0, 0))
        )
        operands.append(fresh)
    message = jax.ShapeDtypeStruct((count, row_count, width + LANES), jnp.bfloat16)
    outs = 1 + len(relays)
    return pl.pallas_call(
        body,
        grid_spec=pltpu.PrefetchScalarGridSpec(
            num_scalar_prefetch=1,
            grid=(count,),
            in_specs=in_specs,
            out_specs=[pl.BlockSpec((1, row_count, width + LANES), lambda k, p: (k, 0, 0))] * outs,
            scratch_shapes=[pltpu.VMEM((1, row_count, width), jnp.bfloat16)],
        ),
        out_shape=[message] * outs,
        name="partial_attention",
        cost_estimate=pl.CostEstimate(
            flops=count * heads * row_count * refs_per_seq * PAGE * HD * 4,
            bytes_accessed=count * row_count * width * 8,
            transcendentals=count * heads * row_count * refs_per_seq * PAGE,
        ),
    )(plan, *operands)


def merge_weights(lses):
    peak = lses[0]
    for lse in lses[1:]:
        peak = jnp.maximum(peak, lse)
    weights = [jnp.exp2(lse - peak) for lse in lses]
    total = weights[0]
    for w in weights[1:]:
        total = total + w
    return [w / total for w in weights], peak + jnp.log2(total)


def merge_pair(plan, mine, incoming, other, *, chips):
    count, _, full = mine.shape
    width = full - LANES
    heads = width // HD
    inputs = [mine, incoming] + ([other] if other is not None else [])

    def body(plan_ref, *rest):
        hbm = rest[: len(inputs)]
        out_ref, mine_ref, incoming_ref, sems = rest[len(inputs) :]
        here = one_of(plan_ref[0], chips, 1)

        @pl.when(here)
        def _():
            parts = [mine_ref, incoming_ref]
            copies = [
                [pltpu.make_async_copy(h.at[k], r.at[k], sems.at[k, n]) for n, (h, r) in enumerate(zip(hbm, parts))]
                for k in range(count)
            ]
            for pair in copies:
                for c in pair:
                    c.start()
            for k in range(count):
                for c in copies[k]:
                    c.wait()
                weights, lse = merge_weights([read_lse(r[k, :, width:], heads) for r in parts])
                for h in range(heads):
                    cols = slice(h * HD, (h + 1) * HD)
                    out_ref[k, :, cols] = sum(
                        r[k, :, cols].astype(jnp.float32) * w[:, h : h + 1]
                        for r, w in zip(parts, weights)
                    ).astype(jnp.bfloat16)
                out_ref[k, :, width:] = lse_block(spread_lse(lse, heads), heads)

        if other is not None:
            @pl.when(jnp.logical_not(here))
            def _():
                copy = pltpu.make_async_copy(hbm[2], out_ref, sems.at[0, 0])
                copy.start()
                copy.wait()

    any_spec = pl.BlockSpec(memory_space=pl.ANY)
    return pl.pallas_call(
        body,
        grid_spec=pltpu.PrefetchScalarGridSpec(
            num_scalar_prefetch=1,
            grid=(1,),
            in_specs=[any_spec] * len(inputs),
            out_specs=pl.BlockSpec(mine.shape, lambda g, p: (0, 0, 0)),
            scratch_shapes=[
                pltpu.VMEM(mine.shape, jnp.bfloat16),
                pltpu.VMEM(mine.shape, jnp.bfloat16),
                pltpu.SemaphoreType.DMA((count, 2)),
            ],
        ),
        out_shape=jax.ShapeDtypeStruct(mine.shape, jnp.bfloat16),
        name="merge_pair",
    )(plan, *inputs)


def merge_final(plan, own, last_in, first_in, choice, *, first, seq_dev, record):
    count, row_count, full = last_in.shape
    width = full - LANES
    heads = width // HD

    def body(plan_ref, own_hbm, last_hbm, *rest):
        first_hbm = rest[: len(first_in)]
        out_ref, own_ref, last_ref, first_ref, sems = rest[len(first_in) :]
        shard = plan_ref[0]
        parts = [own_ref, last_ref, first_ref]

        def copy(source, n, k):
            return pltpu.make_async_copy(source, parts[n].at[k], sems.at[n, k])

        for k in range(count):
            copy(own_hbm.at[first + k], 0, k).start()
            copy(last_hbm.at[k], 1, k).start()
            for n, r in enumerate(first_hbm):
                @pl.when(one_of(shard, choice, n))
                def _(r=r, k=k):
                    copy(r.at[k], 2, k).start()
        for k in range(count):
            for n, r in enumerate((own_hbm, last_hbm, first_hbm[0])):
                copy(r.at[k], n, k).wait()
            weights, _ = merge_weights([read_lse(r[k, :, width:], heads) for r in parts])
            row = lax.broadcasted_iota(jnp.int32, (row_count, HD), 0)
            flag = plan_ref[2 + (shard * seq_dev + first + k) * record + record - 1]
            live = row < jnp.where(flag == 1, row_count, 1)
            for h in range(heads):
                cols = slice(h * HD, (h + 1) * HD)
                total = sum(
                    r[k, :, cols].astype(jnp.float32) * w[:, h : h + 1]
                    for r, w in zip(parts, weights)
                )
                out_ref[k, :, cols] = jnp.where(live, total, 0.0).astype(jnp.bfloat16)

    any_spec = pl.BlockSpec(memory_space=pl.ANY)
    return pl.pallas_call(
        body,
        grid_spec=pltpu.PrefetchScalarGridSpec(
            num_scalar_prefetch=1,
            grid=(1,),
            in_specs=[any_spec] * (2 + len(first_in)),
            out_specs=pl.BlockSpec((count, row_count, width), lambda g, p: (0, 0, 0)),
            scratch_shapes=[pltpu.VMEM(last_in.shape, jnp.bfloat16)] * 3
            + [pltpu.SemaphoreType.DMA((3, count))],
        ),
        out_shape=jax.ShapeDtypeStruct((count, row_count, width), jnp.bfloat16),
        name="merge_final",
    )(plan, own, last_in, *first_in)


CHUNKS = 2
BLOCK_ROWS = 512


def own_columns(core_of, queries, parts, chunk):
    seqs, row_count, full = queries.shape
    width = full // parts

    def body(core_ref, *refs):
        count = len(refs) // 2
        for k in range(count):
            refs[count + k][...] = refs[k][...]

    pieces = seqs // chunk
    return pl.pallas_call(
        body,
        grid_spec=pltpu.PrefetchScalarGridSpec(
            num_scalar_prefetch=1,
            grid=(chunk,),
            in_specs=[
                pl.BlockSpec((1, row_count, width), lambda k, c, n=n: (n * chunk + k, 0, c[0]))
                for n in range(pieces)
            ],
            out_specs=[
                pl.BlockSpec((1, row_count, width), lambda k, c: (k, 0, 0)) for _ in range(pieces)
            ],
        ),
        out_shape=[
            jax.ShapeDtypeStruct((chunk, row_count, width), queries.dtype) for _ in range(pieces)
        ],
        name="own_columns",
    )(core_of, *([queries] * pieces))


def place_columns(core_of, own, other, whole, *, first, seqs):
    count, row_count, width = own.shape

    def body(core_ref, own_ref, other_ref, *rest):
        out_ref = rest[-1]

        @pl.when(core_ref[0] == 0)
        def _():
            out_ref[:, :, :width] = own_ref[...]
            out_ref[:, :, width:] = other_ref[...]

        @pl.when(core_ref[0] != 0)
        def _():
            out_ref[:, :, :width] = other_ref[...]
            out_ref[:, :, width:] = own_ref[...]

    block = pl.BlockSpec((1, row_count, width), lambda k, c: (k, 0, 0))
    operands = [own, other]
    specs = [block, block]
    aliases = {}
    if whole is not None:
        operands.append(whole)
        specs.append(pl.BlockSpec(memory_space=pl.ANY))
        aliases = {3: 0}
    return pl.pallas_call(
        body,
        grid_spec=pltpu.PrefetchScalarGridSpec(
            num_scalar_prefetch=1,
            grid=(count,),
            in_specs=specs,
            out_specs=pl.BlockSpec((1, row_count, 2 * width), lambda k, c: (first + k, 0, 0)),
        ),
        out_shape=jax.ShapeDtypeStruct((seqs, row_count, 2 * width), own.dtype),
        input_output_aliases=aliases,
        name="place_columns",
    )(core_of, *operands)


def queries_travel(queries, new_kv, kv_pages, page_table, cached_len, is_prefill):
    shards = lax.axis_size("seq")
    sub_count = lax.axis_size("sub")
    owners = shards * sub_count
    shard = lax.axis_index("seq")
    core = lax.axis_index("sub")
    seq_dev = queries.shape[0]
    pages_dev = kv_pages.shape[0]
    part_width = kv_pages.shape[3] // sub_count
    picks = -(-page_table.shape[1] // owners)
    record = 2 * sub_count * picks + 1
    chunk = seq_dev // CHUNKS
    firsts = [n * chunk for n in range(CHUNKS)]

    core_of = core.astype(jnp.int32)[None]
    own_queries = own_columns(core_of, queries, sub_count, chunk)
    *own_queries, later_pages = lax.optimization_barrier((*own_queries, kv_pages))
    plan = page_plan(
        page_table, cached_len, is_prefill, shard, core, pages_dev, sub_count, picks
    )

    twin = lax.dynamic_slice_in_dim(later_pages, (1 - core) * part_width, part_width, 3)
    twin_pages = lax.ppermute(twin, "sub", [(0, 1), (1, 0)])
    fresh = jnp.transpose(
        lax.dynamic_slice_in_dim(new_kv, core * part_width, part_width, 3), (2, 0, 1, 3)
    )

    whole_width = queries.shape[2] // sub_count
    common = dict(width=whole_width, seq_dev=seq_dev, picks=picks, sub_count=sub_count)

    def attend(n, sources, choice, homes, relays):
        return partial_attention(
            plan, sources, choice, homes, kv_pages, twin_pages, None, relays,
            count=chunk, first=firsts[n], **common
        )

    def move(array, pairs):
        return lax.ppermute(array, "seq", pairs)

    up = [(0, 1), (1, 2), (2, 3)]
    down = [(3, 2), (2, 1), (1, 0)]
    outward = [(2, 3), (1, 0)]
    inward = [(3, 2), (0, 1)]
    across = [(1, 2), (2, 1)]
    ends = [(3, 0), (0, 3)]
    inner = (0, 1, 1, 0)
    arrived = {}
    for n in range(CHUNKS):
        right1 = move(own_queries[n], up)
        left1 = move(own_queries[n], down)
        one, pay_right, pay_left = attend(
            n, [right1, left1], (1, 1, 0, 0), (1, 2, 1, 2), ((-1, 0, 0, 0), (1, 1, 1, -1))
        )
        right2 = move(pay_right, up)
        left2 = move(pay_left, down)
        two, pay = attend(n, [right2, left2], (1, 1, 0, 0), (2, 3, 0, 1), ((-1, 1, 0, -1),))
        third = move(pay, outward + inward)
        crossed = move(two, across)
        (three,) = attend(n, [third, left1, right1], (0, 2, 1, 0), (3, 0, 3, 0), ())
        joined = merge_pair(plan, one, third, three, chips=inner)
        final = move(joined, across + ends)
        paired = merge_pair(plan, three, crossed, None, chips=inner)
        home = move(paired, outward)
        arrived[n] = (final, [home, right2, left2])
    (own,) = partial_attention(
        plan, [queries], (0,) * shards, tuple(range(shards)), kv_pages, twin_pages, fresh, (),
        count=seq_dev, first=0, **common
    )
    outs = []
    for n in range(CHUNKS):
        final, firsts_in = arrived[n]
        outs.append(
            merge_final(
                plan, own, final, firsts_in, (0, 1, 2, 0),
                first=firsts[n], seq_dev=seq_dev, record=record,
            )
        )
    whole = None
    for n in range(CHUNKS):
        other = lax.ppermute(outs[n], "sub", [(0, 1), (1, 0)])
        whole = place_columns(core_of, outs[n], other, whole, first=firsts[n], seqs=seq_dev)
    return whole


def can_travel(shards, sub_count, seq_dev, query_width, page_count):
    heads = query_width // sub_count // HD
    spread = page_count >= shards * sub_count and shards == 4 and sub_count == 2
    return spread and 3 * heads <= LANES and seq_dev % CHUNKS == 0


def solution(mesh):
    placed = (
        P(("groups", "seq"), None, "head"),
        P(("groups", "seq"), None, None, "head"),
        P(("groups", "seq", "sub"), None, None, "head"),
        P("groups", None),
        P("groups"),
        P("groups"),
    )
    shards = mesh.shape["seq"]

    def placed_map(body):
        return jax.shard_map(
            body,
            mesh=mesh,
            in_specs=placed,
            out_specs=P(("groups", "seq"), None, "head"),
            check_vma=False,
        )

    def run(queries, new_kv, kv_pages, page_table, cached_len, is_prefill):
        args = (queries, new_kv, kv_pages, page_table, cached_len, is_prefill)
        seq_dev = queries.shape[0] // (mesh.shape["groups"] * shards)
        width = queries.shape[2] // mesh.shape["head"]
        if not can_travel(shards, mesh.shape["sub"], seq_dev, width, page_table.shape[1]):
            return placed_map(pages_travel)(*args)

        return placed_map(queries_travel)(*args)

    return run
```

```python
import jax
import jax.numpy as jnp
from jax import lax
from jax.experimental import pallas as pl
from jax.experimental.pallas import tpu as pltpu
from jax.sharding import PartitionSpec as P


HD = 128
PAGE = 128


NEG_FILL = -1e30


def partial_softmax(
    query_heads, cache_keys, cache_values, cache_valid, fresh_keys, fresh_values, fresh_valid
):
    score_scale = HD ** (-0.5)
    cache_scores = (
        jnp.einsum("rkgd,nkd->kgrn", query_heads, cache_keys, preferred_element_type=jnp.float32)
        * score_scale
    )
    fresh_scores = (
        jnp.einsum("rkgd,jkd->kgrj", query_heads, fresh_keys, preferred_element_type=jnp.float32)
        * score_scale
    )
    cache_mask = cache_valid[None, None, None, :]
    fresh_mask = fresh_valid[None, None, :, :]
    peak = jnp.maximum(
        jnp.max(jnp.where(cache_mask, cache_scores, NEG_FILL), axis=-1),
        jnp.max(jnp.where(fresh_mask, fresh_scores, NEG_FILL), axis=-1),
    )
    cache_weights = jnp.where(cache_mask, jnp.exp(cache_scores - peak[..., None]), 0.0)
    fresh_weights = jnp.where(fresh_mask, jnp.exp(fresh_scores - peak[..., None]), 0.0)
    weight_sum = jnp.sum(cache_weights, axis=-1) + jnp.sum(fresh_weights, axis=-1)
    numerator = jnp.einsum(
        "kgrn,nkd->kgrd",
        cache_weights.astype(jnp.bfloat16),
        cache_values,
        preferred_element_type=jnp.float32,
    )
    numerator = numerator + jnp.einsum(
        "kgrj,jkd->kgrd",
        fresh_weights.astype(jnp.bfloat16),
        fresh_values,
        preferred_element_type=jnp.float32,
    )
    return (peak, weight_sum, numerator)


def attend_all(
    query_block, fresh_block, received, fetch_index, page_here, lengths, live_rows, causal, fresh_on
):
    kv_width = received.shape[-1]
    heads_kv = kv_width // HD
    row_count = query_block.shape[1]
    group_size = query_block.shape[2] // kv_width
    page_count = fetch_index.shape[1]
    positions = jnp.arange(page_count * PAGE, dtype=jnp.int32)

    def one_sequence(inputs):
        query_rows, fresh_rows, index_row, here_row, length, live_row = inputs
        fetched = jnp.take(received, index_row, axis=0)
        cache_keys = fetched[:, 0].reshape(page_count * PAGE, heads_kv, HD)
        cache_values = fetched[:, 1].reshape(page_count * PAGE, heads_kv, HD)
        page_mask = jnp.broadcast_to(here_row[:, None], (page_count, PAGE)).reshape(
            page_count * PAGE
        )
        cache_valid = page_mask & (positions < length)
        query_heads = query_rows.reshape(row_count, heads_kv, group_size, HD)
        fresh_keys = fresh_rows[:, 0].reshape(row_count, heads_kv, HD)
        fresh_values = fresh_rows[:, 1].reshape(row_count, heads_kv, HD)
        fresh_valid = causal & live_row[:, None] & fresh_on
        return partial_softmax(
            query_heads,
            cache_keys,
            cache_values,
            cache_valid,
            fresh_keys,
            fresh_values,
            fresh_valid,
        )

    return lax.map(
        one_sequence, (query_block, fresh_block, fetch_index, page_here, lengths, live_rows)
    )


def finish(weight_sum, numerator, live_rows):
    unused_rows = 1.0 - live_rows.astype(jnp.float32)
    attended = numerator / (weight_sum + unused_rows[:, None, None, :])[..., None]
    attended = jnp.where(live_rows[:, None, None, :, None], attended, 0.0)
    seq_dev, heads_kv, group_size, row_count, head_dim = attended.shape
    return (
        jnp.transpose(attended, (0, 3, 1, 2, 4))
        .reshape(seq_dev, row_count, heads_kv * group_size * head_dim)
        .astype(jnp.bfloat16)
    )


def pages_travel(queries, new_kv, kv_pages, page_table, cached_len, is_prefill):
    seq_shards = lax.axis_size("seq")
    sub_count = lax.axis_size("sub")
    owners = seq_shards * sub_count
    seq_index = lax.axis_index("seq")
    core_index = lax.axis_index("sub")
    owner_self = seq_index * sub_count + core_index
    seq_dev, row_count, query_width = queries.shape
    pages_dev = kv_pages.shape[0]
    kv_width = kv_pages.shape[3]
    page_count = page_table.shape[1]
    entries = seq_dev * page_count
    capacity = (entries + owners - 1) // owners
    table_rows = page_table.reshape(seq_shards, entries)
    holder = jnp.where(table_rows >= 0, table_rows // pages_dev, -1)
    slot_of = jnp.where(table_rows >= 0, table_rows % pages_dev, 0)
    owned_here = holder == owner_self
    rank_among = jnp.cumsum(owned_here.astype(jnp.int32), axis=1) - 1
    picked = owned_here[:, :, None] & (
        rank_among[:, :, None] == jnp.arange(capacity, dtype=jnp.int32)[None, None, :]
    )
    send_slots = jnp.sum(jnp.where(picked, slot_of[:, :, None], 0), axis=1).reshape(
        seq_shards * capacity
    )
    first_seq = seq_index * seq_dev
    my_table = lax.dynamic_slice_in_dim(page_table, first_seq, seq_dev, 0)
    my_lengths = lax.dynamic_slice_in_dim(cached_len, first_seq, seq_dev, 0)
    my_flags = lax.dynamic_slice_in_dim(is_prefill, first_seq, seq_dev, 0)
    flat_table = my_table.reshape(entries)
    my_holder = jnp.where(flat_table >= 0, flat_table // pages_dev, -1)
    entry_order = jnp.arange(entries, dtype=jnp.int32)
    earlier = (my_holder[:, None] == my_holder[None, :]) & (
        entry_order[None, :] < entry_order[:, None]
    )
    my_rank = jnp.sum(earlier.astype(jnp.int32), axis=1)
    row_ids = jnp.arange(row_count, dtype=jnp.int32)
    live_rows = (my_flags[:, None] == 1) | (row_ids[None, :] == 0)
    causal = row_ids[None, :] <= row_ids[:, None]
    part_width = kv_width // sub_count
    split_pages = kv_pages.reshape(pages_dev, 2, PAGE, sub_count, part_width)
    chosen = jnp.take(split_pages, send_slots, axis=0).reshape(
        seq_shards, capacity, 2, PAGE, sub_count, part_width
    )
    outgoing = jnp.moveaxis(chosen, 4, 1).reshape(owners, capacity, 2, PAGE, part_width)
    received = lax.all_to_all(
        outgoing, ("seq", "sub"), split_axis=0, concat_axis=0, tiled=True
    ).reshape(owners * capacity, 2, PAGE, part_width)
    present = flat_table >= 0
    fetch_index = jnp.where(present, my_holder * capacity + my_rank, 0)
    query_part = query_width // sub_count
    my_queries = lax.dynamic_slice_in_dim(queries, core_index * query_part, query_part, 2)
    my_fresh = lax.dynamic_slice_in_dim(new_kv, core_index * part_width, part_width, 3)
    _, weight_sum, numerator = attend_all(
        my_queries,
        my_fresh,
        received,
        fetch_index.reshape(seq_dev, page_count),
        present.reshape(seq_dev, page_count),
        my_lengths,
        live_rows,
        causal,
        core_index >= 0,
    )
    own_heads = finish(weight_sum, numerator, live_rows)
    return lax.all_gather(own_heads, "sub", axis=2, tiled=True)


LOG2E = 1.4426950408889634
LANES = 128
NO_KEY = -1e30


def page_plan(page_table, cached_len, is_prefill, shard, core, pages_dev, sub_count, picks):
    seqs, page_count = page_table.shape
    present = page_table >= 0
    owner = jnp.where(present, page_table // pages_dev, -1)
    slot = jnp.where(present, page_table % pages_dev, 0)
    page_ids = jnp.arange(page_count, dtype=jnp.int32)
    keys_here = jnp.clip(cached_len[:, None] - page_ids[None, :] * PAGE, 0, PAGE)
    before = page_ids[None, :] < page_ids[:, None]
    same = owner[:, :, None] == owner[:, None, :]
    rank = jnp.sum((same & before[None]).astype(jnp.int32), axis=2)
    cores = (core + jnp.arange(sub_count, dtype=jnp.int32)) % sub_count
    wanted = shard * sub_count + cores
    picked = (owner[:, None, None, :] == wanted[None, :, None, None]) & (
        rank[:, None, None, :] == jnp.arange(picks, dtype=jnp.int32)[None, None, :, None]
    )
    slots = jnp.sum(jnp.where(picked, slot[:, None, None, :], 0), axis=3)
    counts = jnp.sum(jnp.where(picked, keys_here[:, None, None, :], 0), axis=3)
    rows = jnp.concatenate(
        [
            slots.reshape(seqs, sub_count * picks),
            counts.reshape(seqs, sub_count * picks),
            is_prefill[:, None].astype(jnp.int32),
        ],
        axis=1,
    )
    return jnp.concatenate([jnp.stack([shard, core]).astype(jnp.int32), rows.reshape(-1)])


def lse_block(lse_tile, heads):
    lane = lax.broadcasted_iota(jnp.int32, lse_tile.shape, 1)
    high = lse_tile.astype(jnp.bfloat16)
    rest = lse_tile - high.astype(jnp.float32)
    middle = rest.astype(jnp.bfloat16)
    low = rest - middle.astype(jnp.float32)
    mixed = jnp.where(
        lane < heads,
        high.astype(jnp.float32),
        jnp.where(lane < 2 * heads, middle.astype(jnp.float32), low),
    )
    return mixed.astype(jnp.bfloat16)


def read_lse(block, heads):
    tile = block.astype(jnp.float32)
    return (
        tile
        + pltpu.roll(tile, LANES - heads, 1)
        + pltpu.roll(tile, LANES - 2 * heads, 1)
    )


def spread_lse(lse, heads):
    lane = lax.broadcasted_iota(jnp.int32, lse.shape, 1)
    return jnp.where(
        lane < heads,
        lse,
        jnp.where(lane < 2 * heads, pltpu.roll(lse, heads, 1), pltpu.roll(lse, 2 * heads, 1)),
    )


def one_of(shard, table, value):
    found = None
    for chip, entry in enumerate(table):
        if entry == value:
            here = shard == chip
            found = here if found is None else found | here
    return found


def by_chip(shard, values):
    picked = values[0]
    for chip in range(1, len(values)):
        if values[chip] != values[chip - 1]:
            picked = jnp.where(shard >= chip, values[chip], picked)
    return picked


def partial_attention(
    plan, sources, choice, homes, pages, twin_pages, fresh, relays, *, count, width, first, seq_dev,
    picks, sub_count
):
    row_count = sources[0].shape[1]
    part_width = twin_pages.shape[3]
    heads_kv = part_width // HD
    heads = width // HD
    group = heads // heads_kv
    refs_per_seq = sub_count * picks
    record = 2 * refs_per_seq + 1
    scale = LOG2E * HD ** (-0.5)
    few = min(row_count, 16)

    def entry(plan_ref, k, column):
        home = by_chip(plan_ref[0], homes)
        return plan_ref[2 + (home * seq_dev + first + k) * record + column]

    chunk = sources[0].shape[0]

    def body(plan_ref, *rest):
        query_refs = rest[: len(sources)]
        pages_hbm, twin_hbm = rest[len(sources) : len(sources) + 2]
        fresh_ref = rest[len(sources) + 2] if fresh is not None else None
        query_ref, page_buf, sems = rest[-3:]
        out_ref = rest[-4 - len(relays)]
        relay_refs = rest[-3 - len(relays) : -3]
        shard = plan_ref[0]
        mine = pl.ds(pl.multiple_of(plan_ref[1] * part_width, LANES), part_width)

        def page_copy(k, n):
            slot = entry(plan_ref, k, n)
            source = pages_hbm.at[slot, :, :, mine] if n < picks else twin_hbm.at[slot]
            return pltpu.make_async_copy(source, page_buf.at[k, n], sems.at[k, n])

        for k in range(count):
            for n in range(refs_per_seq):
                page_copy(k, n).start()

        def one(k, carry):
            attend_one(k)
            return carry

        def attend_one(k):
            counts = [entry(plan_ref, k, refs_per_seq + n) for n in range(refs_per_seq)]
            flag = entry(plan_ref, k, 2 * refs_per_seq)
            for n in range(len(sources)):
                if fresh is not None:
                    chosen = k // chunk == n
                else:
                    chosen = one_of(shard, choice, n)

                @pl.when(chosen)
                def _(n=n):
                    query_ref[...] = query_refs[n][k % chunk, :, :width]

            for relay, relay_ref in zip(relays, relay_refs):
                for n in range(len(sources)):
                    if n in relay:
                        @pl.when(one_of(shard, relay, n))
                        def _(n=n, relay_ref=relay_ref):
                            relay_ref[k, :, :width] = query_refs[n][k, :, :width]

            for n in range(refs_per_seq):
                page_copy(k, n).wait()

            @pl.when(flag == 1)
            def _():
                attend(k, counts, row_count, row_count)

            @pl.when(flag != 1)
            def _():
                attend(k, counts, few, 1)
                if few < row_count:
                    out_ref[k, few:, :] = jnp.zeros(
                        (row_count - few, width + LANES), jnp.bfloat16
                    )

            for relay, relay_ref in zip(relays, relay_refs):
                @pl.when(one_of(shard, relay, -1))
                def _(relay_ref=relay_ref):
                    relay_ref[k] = out_ref[k]

        def attend(k, counts, rows, live_rows):
            lane = lax.broadcasted_iota(jnp.int32, (rows, LANES), 1)
            tile = jnp.zeros((rows, LANES), jnp.float32)
            per_block = max(1, min(group, BLOCK_ROWS // rows))
            stacked = per_block * rows
            key_lane = lax.broadcasted_iota(jnp.int32, (stacked, PAGE), 1)
            for h in range(heads_kv):
                cols = slice(h * HD, (h + 1) * HD)
                keys = jnp.concatenate([page_buf[k, n, 0, :, cols] for n in range(refs_per_seq)], axis=0)
                values = jnp.concatenate([page_buf[k, n, 1, :, cols] for n in range(refs_per_seq)], axis=0)
                for g0 in range(0, group, per_block):
                    base = h * group + g0
                    q = jnp.concatenate(
                        [
                            query_ref[:rows, (base + g) * HD : (base + g + 1) * HD]
                            for g in range(per_block)
                        ],
                        axis=0,
                    )
                    s = lax.dot_general(
                        q, keys, (((1,), (1,)), ((), ())), preferred_element_type=jnp.float32
                    )
                    scores = [
                        jnp.where(
                            key_lane < counts[n], s[:, n * PAGE : (n + 1) * PAGE] * scale, NO_KEY
                        )
                        for n in range(refs_per_seq)
                    ]
                    peak = scores[0]
                    for x in scores[1:]:
                        peak = jnp.maximum(peak, x)
                    peak = jnp.max(peak, axis=1, keepdims=True)
                    if fresh is not None:
                        s = lax.dot_general(
                            q,
                            fresh_ref[0, k, :, cols],
                            (((1,), (1,)), ((), ())),
                            preferred_element_type=jnp.float32,
                        )
                        row = lax.broadcasted_iota(jnp.int32, (stacked, row_count), 0) % rows
                        col = lax.broadcasted_iota(jnp.int32, (stacked, row_count), 1)
                        new_scores = jnp.where(
                            (col <= row) & (col < live_rows), s * scale, NO_KEY
                        )
                        peak = jnp.maximum(peak, jnp.max(new_scores, axis=1, keepdims=True))
                    weights = [jnp.exp2(x - peak) for x in scores]
                    sums = weights[0]
                    for w in weights[1:]:
                        sums = sums + w
                    weight_sum = jnp.sum(sums, axis=1, keepdims=True)
                    numerator = lax.dot_general(
                        jnp.concatenate([w.astype(jnp.bfloat16) for w in weights], axis=1),
                        values,
                        (((1,), (0,)), ((), ())),
                        preferred_element_type=jnp.float32,
                    )
                    if fresh is not None:
                        w = jnp.exp2(new_scores - peak)
                        weight_sum = weight_sum + jnp.sum(w, axis=1, keepdims=True)
                        numerator = numerator + lax.dot_general(
                            w.astype(jnp.bfloat16),
                            fresh_ref[1, k, :, cols],
                            (((1,), (0,)), ((), ())),
                            preferred_element_type=jnp.float32,
                        )
                    attended = (numerator / weight_sum).astype(jnp.bfloat16)
                    lse = peak + jnp.log2(weight_sum)
                    for g in range(per_block):
                        head = base + g
                        part = slice(g * rows, (g + 1) * rows)
                        out_ref[k, :rows, head * HD : (head + 1) * HD] = attended[part]
                        spots = (lane == head) | (lane == head + heads) | (lane == head + 2 * heads)
                        tile = jnp.where(spots, lse[part], tile)
            out_ref[k, :rows, width:] = lse_block(tile, heads)

        lax.fori_loop(0, count, one, 0)

    vmem = pl.BlockSpec(memory_space=pltpu.VMEM)
    hbm = pl.BlockSpec(memory_space=pltpu.HBM)
    operands = [in_vmem(x) for x in sources] + [in_hbm(pages), in_hbm(twin_pages)]
    in_specs = [vmem] * len(sources) + [hbm, hbm]
    if fresh is not None:
        operands.append(fresh)
        in_specs.append(vmem)
    outs = 1 + len(relays)
    return pl.pallas_call(
        body,
        in_specs=[pl.BlockSpec(memory_space=pltpu.SMEM)] + in_specs,
        out_specs=[vmem] * outs,
        out_shape=[pltpu.VMEM((count, row_count, width + LANES), jnp.bfloat16)] * outs,
        scratch_shapes=[
            pltpu.VMEM((row_count, width), jnp.bfloat16),
            pltpu.VMEM((count, refs_per_seq, 2, PAGE, part_width), jnp.bfloat16),
            pltpu.SemaphoreType.DMA((count, refs_per_seq)),
        ],
        name="partial_attention",
        compiler_params=pltpu.CompilerParams(vmem_limit_bytes=24 << 20),
        cost_estimate=pl.CostEstimate(
            flops=count * heads * row_count * refs_per_seq * PAGE * HD * 4,
            bytes_accessed=count * row_count * width * 8,
            transcendentals=count * heads * row_count * refs_per_seq * PAGE,
        ),
    )(plan, *operands)


def in_hbm(array):
    return pltpu.with_memory_space_constraint(array, pltpu.HBM)


def in_vmem(array):
    return pltpu.with_memory_space_constraint(array, pltpu.VMEM)


def merge_weights(lses):
    peak = lses[0]
    for lse in lses[1:]:
        peak = jnp.maximum(peak, lse)
    weights = [jnp.exp2(lse - peak) for lse in lses]
    total = weights[0]
    for w in weights[1:]:
        total = total + w
    return [w / total for w in weights], peak + jnp.log2(total)


def merge_pair(plan, mine, incoming, other, *, chips):
    count, _, full = mine.shape
    width = full - LANES
    heads = width // HD
    inputs = [mine, incoming] + ([other] if other is not None else [])

    def body(plan_ref, *rest):
        out_ref = rest[len(inputs)]
        here = one_of(plan_ref[0], chips, 1)

        @pl.when(here)
        def _():
            parts = rest[:2]
            for k in range(count):
                weights, lse = merge_weights([read_lse(r[k, :, width:], heads) for r in parts])
                for h in range(heads):
                    cols = slice(h * HD, (h + 1) * HD)
                    out_ref[k, :, cols] = sum(
                        r[k, :, cols].astype(jnp.float32) * w[:, h : h + 1]
                        for r, w in zip(parts, weights)
                    ).astype(jnp.bfloat16)
                out_ref[k, :, width:] = lse_block(spread_lse(lse, heads), heads)

        if other is not None:
            @pl.when(jnp.logical_not(here))
            def _():
                out_ref[...] = rest[2][...]

    vmem = pl.BlockSpec(memory_space=pltpu.VMEM)
    return pl.pallas_call(
        body,
        in_specs=[pl.BlockSpec(memory_space=pltpu.SMEM)] + [vmem] * len(inputs),
        out_specs=vmem,
        out_shape=pltpu.VMEM(mine.shape, jnp.bfloat16),
        name="merge_pair",
        compiler_params=pltpu.CompilerParams(vmem_limit_bytes=16 << 20),
    )(plan, *[in_vmem(x) for x in inputs])


def merge_final(plan, own, last_in, first_in, choice, *, first, seq_dev, record):
    count, row_count, full = last_in.shape
    width = full - LANES
    heads = width // HD

    def body(plan_ref, own_ref, last_ref, *rest):
        first_refs = rest[: len(first_in)]
        out_ref = rest[len(first_in)]
        shard = plan_ref[0]

        def finish(first_ref):
            for k in range(count):
                parts = [own_ref.at[first + k], last_ref.at[k], first_ref.at[k]]
                weights, _ = merge_weights([read_lse(r[:, width:], heads) for r in parts])
                row = lax.broadcasted_iota(jnp.int32, (row_count, HD), 0)
                flag = plan_ref[2 + (shard * seq_dev + first + k) * record + record - 1]
                live = row < jnp.where(flag == 1, row_count, 1)
                for h in range(heads):
                    cols = slice(h * HD, (h + 1) * HD)
                    total = sum(
                        r[:, cols].astype(jnp.float32) * w[:, h : h + 1]
                        for r, w in zip(parts, weights)
                    )
                    out_ref[k, :, cols] = jnp.where(live, total, 0.0).astype(jnp.bfloat16)

        for n, r in enumerate(first_refs):
            @pl.when(one_of(shard, choice, n))
            def _(r=r):
                finish(r)

    vmem = pl.BlockSpec(memory_space=pltpu.VMEM)
    operands = [own, last_in, *first_in]
    return pl.pallas_call(
        body,
        in_specs=[pl.BlockSpec(memory_space=pltpu.SMEM)] + [vmem] * len(operands),
        out_specs=vmem,
        out_shape=pltpu.VMEM((count, row_count, width), jnp.bfloat16),
        name="merge_final",
        compiler_params=pltpu.CompilerParams(vmem_limit_bytes=16 << 20),
    )(plan, *[in_vmem(x) for x in operands])


CHUNKS = 2
BLOCK_ROWS = 512


def own_columns(core_of, queries, parts, first, count):
    _, row_count, full = queries.shape
    width = full // parts

    def body(core_ref, source, out_ref, sem):
        cols = pl.ds(pl.multiple_of(core_ref[0] * width, LANES), width)
        copy = pltpu.make_async_copy(source.at[first : first + count, :, cols], out_ref, sem)
        copy.start()
        copy.wait()

    return pl.pallas_call(
        body,
        in_specs=[
            pl.BlockSpec(memory_space=pltpu.SMEM),
            pl.BlockSpec(memory_space=pltpu.HBM),
        ],
        out_specs=pl.BlockSpec(memory_space=pltpu.VMEM),
        out_shape=pltpu.VMEM((count, row_count, width), queries.dtype),
        scratch_shapes=[pltpu.SemaphoreType.DMA],
        name="own_columns",
        compiler_params=pltpu.CompilerParams(vmem_limit_bytes=16 << 20),
    )(core_of, in_hbm(queries))


def place_columns(core_of, own, other, whole, *, first, seqs):
    count, row_count, width = own.shape

    def body(core_ref, own_ref, other_ref, *rest):
        out_ref, sems = rest[-2:]
        copies = []
        for n, r in enumerate((own_ref, other_ref)):
            core = core_ref[0] if n == 0 else 1 - core_ref[0]
            cols = pl.ds(pl.multiple_of(core * width, LANES), width)
            target = out_ref.at[first : first + count, :, cols]
            copies.append(pltpu.make_async_copy(r, target, sems.at[n]))
        for c in copies:
            c.start()
        for c in copies:
            c.wait()

    vmem = pl.BlockSpec(memory_space=pltpu.VMEM)
    operands = [in_vmem(own), in_vmem(other)]
    specs = [vmem, vmem]
    aliases = {}
    if whole is not None:
        operands.append(whole)
        specs.append(pl.BlockSpec(memory_space=pl.ANY))
        aliases = {3: 0}
    return pl.pallas_call(
        body,
        in_specs=[pl.BlockSpec(memory_space=pltpu.SMEM)] + specs,
        out_specs=pl.BlockSpec(memory_space=pl.ANY),
        out_shape=jax.ShapeDtypeStruct((seqs, row_count, 2 * width), own.dtype),
        scratch_shapes=[pltpu.SemaphoreType.DMA((2,))],
        input_output_aliases=aliases,
        name="place_columns",
        compiler_params=pltpu.CompilerParams(vmem_limit_bytes=16 << 20),
    )(core_of, *operands)


def queries_travel(queries, new_kv, kv_pages, page_table, cached_len, is_prefill):
    shards = lax.axis_size("seq")
    sub_count = lax.axis_size("sub")
    owners = shards * sub_count
    shard = lax.axis_index("seq")
    core = lax.axis_index("sub")
    seq_dev = queries.shape[0]
    pages_dev = kv_pages.shape[0]
    part_width = kv_pages.shape[3] // sub_count
    picks = -(-page_table.shape[1] // owners)
    record = 2 * sub_count * picks + 1
    chunk = seq_dev // CHUNKS
    firsts = [n * chunk for n in range(CHUNKS)]

    core_of = core.astype(jnp.int32)[None]
    own_queries = []
    for n in range(CHUNKS):
        own_queries.append(own_columns(core_of, queries, sub_count, firsts[n], chunk))
    _, later_pages = lax.optimization_barrier((own_queries[-1], kv_pages))
    plan = page_plan(
        page_table, cached_len, is_prefill, shard, core, pages_dev, sub_count, picks
    )

    twin = lax.dynamic_slice_in_dim(later_pages, (1 - core) * part_width, part_width, 3)
    twin_pages = lax.ppermute(twin, "sub", [(0, 1), (1, 0)])
    fresh = jnp.transpose(
        lax.dynamic_slice_in_dim(new_kv, core * part_width, part_width, 3), (2, 0, 1, 3)
    )

    whole_width = queries.shape[2] // sub_count
    common = dict(width=whole_width, seq_dev=seq_dev, picks=picks, sub_count=sub_count)

    def attend(n, sources, choice, homes, relays):
        return partial_attention(
            plan, sources, choice, homes, kv_pages, twin_pages, None, relays,
            count=chunk, first=firsts[n], **common
        )

    def move(array, pairs):
        return lax.ppermute(array, "seq", pairs)

    up = [(0, 1), (1, 2), (2, 3)]
    down = [(3, 2), (2, 1), (1, 0)]
    outward = [(2, 3), (1, 0)]
    inward = [(3, 2), (0, 1)]
    across = [(1, 2), (2, 1)]
    ends = [(3, 0), (0, 3)]
    inner = (0, 1, 1, 0)
    arrived = {}
    for n in range(CHUNKS):
        right1 = move(own_queries[n], up)
        left1 = move(own_queries[n], down)
        one, pay_right, pay_left = attend(
            n, [right1, left1], (1, 1, 0, 0), (1, 2, 1, 2), ((-1, 0, 0, 0), (1, 1, 1, -1))
        )
        right2 = move(pay_right, up)
        left2 = move(pay_left, down)
        two, pay = attend(n, [right2, left2], (1, 1, 0, 0), (2, 3, 0, 1), ((-1, 1, 0, -1),))
        third = move(pay, outward + inward)
        crossed = move(two, across)
        (three,) = attend(n, [third, left1, right1], (0, 2, 1, 0), (3, 0, 3, 0), ())
        joined = merge_pair(plan, one, third, three, chips=inner)
        final = move(joined, across + ends)
        paired = merge_pair(plan, three, crossed, None, chips=inner)
        home = move(paired, outward)
        arrived[n] = (final, [home, right2, left2])
    (own,) = partial_attention(
        plan, own_queries, (0,) * shards, tuple(range(shards)), kv_pages, twin_pages, fresh, (),
        count=seq_dev, first=0, **common
    )
    outs = []
    for n in range(CHUNKS):
        final, firsts_in = arrived[n]
        outs.append(
            merge_final(
                plan, own, final, firsts_in, (0, 1, 2, 0),
                first=firsts[n], seq_dev=seq_dev, record=record,
            )
        )
    whole = None
    for n in range(CHUNKS):
        other = lax.ppermute(outs[n], "sub", [(0, 1), (1, 0)])
        whole = place_columns(core_of, outs[n], other, whole, first=firsts[n], seqs=seq_dev)
    return whole


def can_travel(shards, sub_count, seq_dev, query_width, page_count):
    heads = query_width // sub_count // HD
    spread = page_count >= shards * sub_count and shards == 4 and sub_count == 2
    return spread and 3 * heads <= LANES and seq_dev % CHUNKS == 0


def solution(mesh):
    placed = (
        P(("groups", "seq"), None, "head"),
        P(("groups", "seq"), None, None, "head"),
        P(("groups", "seq", "sub"), None, None, "head"),
        P("groups", None),
        P("groups"),
        P("groups"),
    )
    shards = mesh.shape["seq"]

    def placed_map(body):
        return jax.shard_map(
            body,
            mesh=mesh,
            in_specs=placed,
            out_specs=P(("groups", "seq"), None, "head"),
            check_vma=False,
        )

    def run(queries, new_kv, kv_pages, page_table, cached_len, is_prefill):
        args = (queries, new_kv, kv_pages, page_table, cached_len, is_prefill)
        seq_dev = queries.shape[0] // (mesh.shape["groups"] * shards)
        width = queries.shape[2] // mesh.shape["head"]
        if not can_travel(shards, mesh.shape["sub"], seq_dev, width, page_table.shape[1]):
            return placed_map(pages_travel)(*args)

        return placed_map(queries_travel)(*args)

    return run
```

```python
import jax
import jax.numpy as jnp
from jax import lax
from jax.experimental import pallas as pl
from jax.experimental.pallas import tpu as pltpu
from jax.sharding import PartitionSpec as P


HD = 128
PAGE = 128


NEG_FILL = -1e30


def partial_softmax(
    query_heads, cache_keys, cache_values, cache_valid, fresh_keys, fresh_values, fresh_valid
):
    score_scale = HD ** (-0.5)
    cache_scores = (
        jnp.einsum("rkgd,nkd->kgrn", query_heads, cache_keys, preferred_element_type=jnp.float32)
        * score_scale
    )
    fresh_scores = (
        jnp.einsum("rkgd,jkd->kgrj", query_heads, fresh_keys, preferred_element_type=jnp.float32)
        * score_scale
    )
    cache_mask = cache_valid[None, None, None, :]
    fresh_mask = fresh_valid[None, None, :, :]
    peak = jnp.maximum(
        jnp.max(jnp.where(cache_mask, cache_scores, NEG_FILL), axis=-1),
        jnp.max(jnp.where(fresh_mask, fresh_scores, NEG_FILL), axis=-1),
    )
    cache_weights = jnp.where(cache_mask, jnp.exp(cache_scores - peak[..., None]), 0.0)
    fresh_weights = jnp.where(fresh_mask, jnp.exp(fresh_scores - peak[..., None]), 0.0)
    weight_sum = jnp.sum(cache_weights, axis=-1) + jnp.sum(fresh_weights, axis=-1)
    numerator = jnp.einsum(
        "kgrn,nkd->kgrd",
        cache_weights.astype(jnp.bfloat16),
        cache_values,
        preferred_element_type=jnp.float32,
    )
    numerator = numerator + jnp.einsum(
        "kgrj,jkd->kgrd",
        fresh_weights.astype(jnp.bfloat16),
        fresh_values,
        preferred_element_type=jnp.float32,
    )
    return (peak, weight_sum, numerator)


def attend_all(
    query_block, fresh_block, received, fetch_index, page_here, lengths, live_rows, causal, fresh_on
):
    kv_width = received.shape[-1]
    heads_kv = kv_width // HD
    row_count = query_block.shape[1]
    group_size = query_block.shape[2] // kv_width
    page_count = fetch_index.shape[1]
    positions = jnp.arange(page_count * PAGE, dtype=jnp.int32)

    def one_sequence(inputs):
        query_rows, fresh_rows, index_row, here_row, length, live_row = inputs
        fetched = jnp.take(received, index_row, axis=0)
        cache_keys = fetched[:, 0].reshape(page_count * PAGE, heads_kv, HD)
        cache_values = fetched[:, 1].reshape(page_count * PAGE, heads_kv, HD)
        page_mask = jnp.broadcast_to(here_row[:, None], (page_count, PAGE)).reshape(
            page_count * PAGE
        )
        cache_valid = page_mask & (positions < length)
        query_heads = query_rows.reshape(row_count, heads_kv, group_size, HD)
        fresh_keys = fresh_rows[:, 0].reshape(row_count, heads_kv, HD)
        fresh_values = fresh_rows[:, 1].reshape(row_count, heads_kv, HD)
        fresh_valid = causal & live_row[:, None] & fresh_on
        return partial_softmax(
            query_heads,
            cache_keys,
            cache_values,
            cache_valid,
            fresh_keys,
            fresh_values,
            fresh_valid,
        )

    return lax.map(
        one_sequence, (query_block, fresh_block, fetch_index, page_here, lengths, live_rows)
    )


def finish(weight_sum, numerator, live_rows):
    unused_rows = 1.0 - live_rows.astype(jnp.float32)
    attended = numerator / (weight_sum + unused_rows[:, None, None, :])[..., None]
    attended = jnp.where(live_rows[:, None, None, :, None], attended, 0.0)
    seq_dev, heads_kv, group_size, row_count, head_dim = attended.shape
    return (
        jnp.transpose(attended, (0, 3, 1, 2, 4))
        .reshape(seq_dev, row_count, heads_kv * group_size * head_dim)
        .astype(jnp.bfloat16)
    )


def pages_travel(queries, new_kv, kv_pages, page_table, cached_len, is_prefill):
    seq_shards = lax.axis_size("seq")
    sub_count = lax.axis_size("sub")
    owners = seq_shards * sub_count
    seq_index = lax.axis_index("seq")
    core_index = lax.axis_index("sub")
    owner_self = seq_index * sub_count + core_index
    seq_dev, row_count, query_width = queries.shape
    pages_dev = kv_pages.shape[0]
    kv_width = kv_pages.shape[3]
    page_count = page_table.shape[1]
    entries = seq_dev * page_count
    capacity = (entries + owners - 1) // owners
    table_rows = page_table.reshape(seq_shards, entries)
    holder = jnp.where(table_rows >= 0, table_rows // pages_dev, -1)
    slot_of = jnp.where(table_rows >= 0, table_rows % pages_dev, 0)
    owned_here = holder == owner_self
    rank_among = jnp.cumsum(owned_here.astype(jnp.int32), axis=1) - 1
    picked = owned_here[:, :, None] & (
        rank_among[:, :, None] == jnp.arange(capacity, dtype=jnp.int32)[None, None, :]
    )
    send_slots = jnp.sum(jnp.where(picked, slot_of[:, :, None], 0), axis=1).reshape(
        seq_shards * capacity
    )
    first_seq = seq_index * seq_dev
    my_table = lax.dynamic_slice_in_dim(page_table, first_seq, seq_dev, 0)
    my_lengths = lax.dynamic_slice_in_dim(cached_len, first_seq, seq_dev, 0)
    my_flags = lax.dynamic_slice_in_dim(is_prefill, first_seq, seq_dev, 0)
    flat_table = my_table.reshape(entries)
    my_holder = jnp.where(flat_table >= 0, flat_table // pages_dev, -1)
    entry_order = jnp.arange(entries, dtype=jnp.int32)
    earlier = (my_holder[:, None] == my_holder[None, :]) & (
        entry_order[None, :] < entry_order[:, None]
    )
    my_rank = jnp.sum(earlier.astype(jnp.int32), axis=1)
    row_ids = jnp.arange(row_count, dtype=jnp.int32)
    live_rows = (my_flags[:, None] == 1) | (row_ids[None, :] == 0)
    causal = row_ids[None, :] <= row_ids[:, None]
    part_width = kv_width // sub_count
    split_pages = kv_pages.reshape(pages_dev, 2, PAGE, sub_count, part_width)
    chosen = jnp.take(split_pages, send_slots, axis=0).reshape(
        seq_shards, capacity, 2, PAGE, sub_count, part_width
    )
    outgoing = jnp.moveaxis(chosen, 4, 1).reshape(owners, capacity, 2, PAGE, part_width)
    received = lax.all_to_all(
        outgoing, ("seq", "sub"), split_axis=0, concat_axis=0, tiled=True
    ).reshape(owners * capacity, 2, PAGE, part_width)
    present = flat_table >= 0
    fetch_index = jnp.where(present, my_holder * capacity + my_rank, 0)
    query_part = query_width // sub_count
    my_queries = lax.dynamic_slice_in_dim(queries, core_index * query_part, query_part, 2)
    my_fresh = lax.dynamic_slice_in_dim(new_kv, core_index * part_width, part_width, 3)
    _, weight_sum, numerator = attend_all(
        my_queries,
        my_fresh,
        received,
        fetch_index.reshape(seq_dev, page_count),
        present.reshape(seq_dev, page_count),
        my_lengths,
        live_rows,
        causal,
        core_index >= 0,
    )
    own_heads = finish(weight_sum, numerator, live_rows)
    return lax.all_gather(own_heads, "sub", axis=2, tiled=True)


LOG2E = 1.4426950408889634
LANES = 128
NO_KEY = -1e30


def page_plan(page_table, cached_len, is_prefill, shard, core, pages_dev, sub_count, picks):
    seqs, page_count = page_table.shape
    present = page_table >= 0
    owner = jnp.where(present, page_table // pages_dev, -1)
    slot = jnp.where(present, page_table % pages_dev, 0)
    page_ids = jnp.arange(page_count, dtype=jnp.int32)
    keys_here = jnp.clip(cached_len[:, None] - page_ids[None, :] * PAGE, 0, PAGE)
    before = page_ids[None, :] < page_ids[:, None]
    same = owner[:, :, None] == owner[:, None, :]
    rank = jnp.sum((same & before[None]).astype(jnp.int32), axis=2)
    cores = (core + jnp.arange(sub_count, dtype=jnp.int32)) % sub_count
    wanted = shard * sub_count + cores
    picked = (owner[:, None, None, :] == wanted[None, :, None, None]) & (
        rank[:, None, None, :] == jnp.arange(picks, dtype=jnp.int32)[None, None, :, None]
    )
    slots = jnp.sum(jnp.where(picked, slot[:, None, None, :], 0), axis=3)
    counts = jnp.sum(jnp.where(picked, keys_here[:, None, None, :], 0), axis=3)
    rows = jnp.concatenate(
        [
            slots.reshape(seqs, sub_count * picks),
            counts.reshape(seqs, sub_count * picks),
            is_prefill[:, None].astype(jnp.int32),
        ],
        axis=1,
    )
    return jnp.concatenate([jnp.stack([shard, core]).astype(jnp.int32), rows.reshape(-1)])


def lse_third(shape, heads):
    lane = lax.broadcasted_iota(jnp.int32, shape, 1)
    return lane % (3 * heads) // heads


def lse_block(lse_tile, heads):
    third = lse_third(lse_tile.shape, heads)
    high = lse_tile.astype(jnp.bfloat16)
    rest = lse_tile - high.astype(jnp.float32)
    middle = rest.astype(jnp.bfloat16)
    low = rest - middle.astype(jnp.float32)
    mixed = jnp.where(
        third == 0,
        high.astype(jnp.float32),
        jnp.where(third == 1, middle.astype(jnp.float32), low),
    )
    return mixed.astype(jnp.bfloat16)


def read_lse(block, heads):
    tile = block.astype(jnp.float32)
    return (
        tile
        + pltpu.roll(tile, LANES - heads, 1)
        + pltpu.roll(tile, LANES - 2 * heads, 1)
    )


def spread_lse(lse, heads):
    third = lse_third(lse.shape, heads)
    return jnp.where(
        third == 0,
        lse,
        jnp.where(third == 1, pltpu.roll(lse, heads, 1), pltpu.roll(lse, 2 * heads, 1)),
    )


def one_of(shard, table, value):
    found = None
    for chip, entry in enumerate(table):
        if entry == value:
            here = shard == chip
            found = here if found is None else found | here
    return found


def by_chip(shard, values):
    picked = values[0]
    for chip in range(1, len(values)):
        if values[chip] != values[chip - 1]:
            picked = jnp.where(shard >= chip, values[chip], picked)
    return picked


def partial_attention(
    plan, sources, choice, homes, pages, twin_pages, fresh, relays, *, count, width, first, seq_dev,
    picks, sub_count
):
    row_count = sources[0].shape[0]
    part_width = twin_pages.shape[3]
    heads_kv = part_width // HD
    heads = width // HD
    group = heads // heads_kv
    refs_per_seq = sub_count * picks
    record = 2 * refs_per_seq + 1
    scale = LOG2E * HD ** (-0.5)
    few = min(row_count, 16)

    def entry(plan_ref, k, column):
        home = by_chip(plan_ref[0], homes)
        return plan_ref[2 + (home * seq_dev + first + k) * record + column]

    total = count * width

    def body(plan_ref, *rest):
        query_refs = rest[: len(sources)]
        pages_hbm, twin_hbm = rest[len(sources) : len(sources) + 2]
        fresh_ref = rest[len(sources) + 2] if fresh is not None else None
        query_ref, result_ref, page_buf, sems = rest[-4:]
        out_ref = rest[-5 - len(relays)]
        relay_refs = rest[-4 - len(relays) : -4]
        shard = plan_ref[0]
        mine = pl.ds(pl.multiple_of(plan_ref[1] * part_width, LANES), part_width)

        def page_copy(k, n):
            slot = entry(plan_ref, k, n)
            source = pages_hbm.at[slot, :, :, mine] if n < picks else twin_hbm.at[slot]
            return pltpu.make_async_copy(source, page_buf.at[k, n], sems.at[k, n])

        for k in range(count):
            for n in range(refs_per_seq):
                page_copy(k, n).start()

        def one(k, carry):
            attend_one(k)
            return carry

        def attend_one(k):
            counts = [entry(plan_ref, k, refs_per_seq + n) for n in range(refs_per_seq)]
            flag = entry(plan_ref, k, 2 * refs_per_seq)
            for j in range(count):
                for n in range(len(sources)):
                    @pl.when((k == j) & one_of(shard, choice, n))
                    def _(n=n, j=j):
                        query_ref[...] = query_refs[n][:, j * width : (j + 1) * width]

            for n in range(refs_per_seq):
                page_copy(k, n).wait()

            @pl.when(flag == 1)
            def _():
                attend(k, counts, row_count, row_count)

            @pl.when(flag != 1)
            def _():
                attend(k, counts, few, 1)
                if few < row_count:
                    result_ref[few:, :] = jnp.zeros((row_count - few, width), jnp.bfloat16)

            for j in range(count):
                @pl.when(k == j)
                def _(j=j):
                    out_ref[:, j * width : (j + 1) * width] = result_ref[...]

        def attend(k, counts, rows, live_rows):
            lane = lax.broadcasted_iota(jnp.int32, (rows, LANES), 1)
            tile = jnp.zeros((rows, LANES), jnp.float32)
            start = k * (3 * heads)
            per_block = max(1, min(group, BLOCK_ROWS // rows))
            stacked = per_block * rows
            key_lane = lax.broadcasted_iota(jnp.int32, (stacked, PAGE), 1)
            for h in range(heads_kv):
                cols = slice(h * HD, (h + 1) * HD)
                keys = jnp.concatenate([page_buf[k, n, 0, :, cols] for n in range(refs_per_seq)], axis=0)
                values = jnp.concatenate([page_buf[k, n, 1, :, cols] for n in range(refs_per_seq)], axis=0)
                for g0 in range(0, group, per_block):
                    base = h * group + g0
                    q = jnp.concatenate(
                        [
                            query_ref[:rows, (base + g) * HD : (base + g + 1) * HD]
                            for g in range(per_block)
                        ],
                        axis=0,
                    )
                    s = lax.dot_general(
                        q, keys, (((1,), (1,)), ((), ())), preferred_element_type=jnp.float32
                    )
                    scores = [
                        jnp.where(
                            key_lane < counts[n], s[:, n * PAGE : (n + 1) * PAGE] * scale, NO_KEY
                        )
                        for n in range(refs_per_seq)
                    ]
                    peak = scores[0]
                    for x in scores[1:]:
                        peak = jnp.maximum(peak, x)
                    peak = jnp.max(peak, axis=1, keepdims=True)
                    if fresh is not None:
                        s = lax.dot_general(
                            q,
                            fresh_ref[0, k, :, cols],
                            (((1,), (1,)), ((), ())),
                            preferred_element_type=jnp.float32,
                        )
                        row = lax.broadcasted_iota(jnp.int32, (stacked, row_count), 0) % rows
                        col = lax.broadcasted_iota(jnp.int32, (stacked, row_count), 1)
                        new_scores = jnp.where(
                            (col <= row) & (col < live_rows), s * scale, NO_KEY
                        )
                        peak = jnp.maximum(peak, jnp.max(new_scores, axis=1, keepdims=True))
                    weights = [jnp.exp2(x - peak) for x in scores]
                    sums = weights[0]
                    for w in weights[1:]:
                        sums = sums + w
                    weight_sum = jnp.sum(sums, axis=1, keepdims=True)
                    numerator = lax.dot_general(
                        jnp.concatenate([w.astype(jnp.bfloat16) for w in weights], axis=1),
                        values,
                        (((1,), (0,)), ((), ())),
                        preferred_element_type=jnp.float32,
                    )
                    if fresh is not None:
                        w = jnp.exp2(new_scores - peak)
                        weight_sum = weight_sum + jnp.sum(w, axis=1, keepdims=True)
                        numerator = numerator + lax.dot_general(
                            w.astype(jnp.bfloat16),
                            fresh_ref[1, k, :, cols],
                            (((1,), (0,)), ((), ())),
                            preferred_element_type=jnp.float32,
                        )
                    attended = (numerator / weight_sum).astype(jnp.bfloat16)
                    lse = peak + jnp.log2(weight_sum)
                    for g in range(per_block):
                        head = base + g
                        part = slice(g * rows, (g + 1) * rows)
                        result_ref[:rows, head * HD : (head + 1) * HD] = attended[part]
                        spot = lane - start - head
                        spots = (spot == 0) | (spot == heads) | (spot == 2 * heads)
                        tile = jnp.where(spots, lse[part], tile)
            here = (lane >= start) & (lane < start + 3 * heads)
            before = out_ref[:rows, total:].astype(jnp.float32)
            block = lse_block(tile, heads).astype(jnp.float32)
            out_ref[:rows, total:] = jnp.where(here, block, before).astype(jnp.bfloat16)

        out_ref[:, total:] = jnp.zeros((row_count, LANES), jnp.bfloat16)
        for relay, relay_ref in zip(relays, relay_refs):
            for n in range(len(sources)):
                if n in relay:
                    @pl.when(one_of(shard, relay, n))
                    def _(n=n, relay_ref=relay_ref):
                        relay_ref[:, :total] = query_refs[n][:, :total]
        lax.fori_loop(0, count, one, 0)
        for relay, relay_ref in zip(relays, relay_refs):
            @pl.when(one_of(shard, relay, -1))
            def _(relay_ref=relay_ref):
                relay_ref[...] = out_ref[...]

    vmem = pl.BlockSpec(memory_space=pltpu.VMEM)
    hbm = pl.BlockSpec(memory_space=pltpu.HBM)
    operands = [in_vmem(x) for x in sources] + [in_hbm(pages), in_hbm(twin_pages)]
    in_specs = [vmem] * len(sources) + [hbm, hbm]
    if fresh is not None:
        operands.append(fresh)
        in_specs.append(vmem)
    outs = 1 + len(relays)
    return pl.pallas_call(
        body,
        in_specs=[pl.BlockSpec(memory_space=pltpu.SMEM)] + in_specs,
        out_specs=[vmem] * outs,
        out_shape=[pltpu.VMEM((row_count, total + LANES), jnp.bfloat16)] * outs,
        scratch_shapes=[
            pltpu.VMEM((row_count, width), jnp.bfloat16),
            pltpu.VMEM((row_count, width), jnp.bfloat16),
            pltpu.VMEM((count, refs_per_seq, 2, PAGE, part_width), jnp.bfloat16),
            pltpu.SemaphoreType.DMA((count, refs_per_seq)),
        ],
        name="partial_attention",
        compiler_params=pltpu.CompilerParams(vmem_limit_bytes=24 << 20),
        cost_estimate=pl.CostEstimate(
            flops=count * heads * row_count * refs_per_seq * PAGE * HD * 4,
            bytes_accessed=count * row_count * width * 8,
            transcendentals=count * heads * row_count * refs_per_seq * PAGE,
        ),
    )(plan, *operands)


def in_hbm(array):
    return pltpu.with_memory_space_constraint(array, pltpu.HBM)


def in_vmem(array):
    return pltpu.with_memory_space_constraint(array, pltpu.VMEM)


def merge_weights(lses):
    peak = lses[0]
    for lse in lses[1:]:
        peak = jnp.maximum(peak, lse)
    weights = [jnp.exp2(lse - peak) for lse in lses]
    total = weights[0]
    for w in weights[1:]:
        total = total + w
    return [w / total for w in weights], peak + jnp.log2(total)


def merge_pair(plan, mine, incoming, other, *, chips, width):
    total = mine.shape[1] - LANES
    heads = width // HD
    inputs = [mine, incoming] + ([other] if other is not None else [])

    def body(plan_ref, *rest):
        out_ref = rest[len(inputs)]
        here = one_of(plan_ref[0], chips, 1)

        @pl.when(here)
        def _():
            parts = rest[:2]
            weights, lse = merge_weights([read_lse(r[:, total:], heads) for r in parts])
            for k in range(total // width):
                for h in range(heads):
                    cols = slice(k * width + h * HD, k * width + (h + 1) * HD)
                    spot = 3 * heads * k + h
                    out_ref[:, cols] = sum(
                        r[:, cols].astype(jnp.float32) * w[:, spot : spot + 1]
                        for r, w in zip(parts, weights)
                    ).astype(jnp.bfloat16)
            out_ref[:, total:] = lse_block(spread_lse(lse, heads), heads)

        if other is not None:
            @pl.when(jnp.logical_not(here))
            def _():
                out_ref[...] = rest[2][...]

    vmem = pl.BlockSpec(memory_space=pltpu.VMEM)
    return pl.pallas_call(
        body,
        in_specs=[pl.BlockSpec(memory_space=pltpu.SMEM)] + [vmem] * len(inputs),
        out_specs=vmem,
        out_shape=pltpu.VMEM(mine.shape, jnp.bfloat16),
        name="merge_pair",
        compiler_params=pltpu.CompilerParams(vmem_limit_bytes=16 << 20),
    )(plan, *[in_vmem(x) for x in inputs])


def merge_final(plan, own, last_in, first_in, choice, *, first, seq_dev, record, width):
    row_count, full = last_in.shape
    total = full - LANES
    count = total // width
    heads = width // HD

    def body(plan_ref, own_ref, last_ref, *rest):
        first_refs = rest[: len(first_in)]
        out_ref = rest[len(first_in)]
        shard = plan_ref[0]

        def finish(first_ref):
            parts = [own_ref, last_ref, first_ref]
            weights, _ = merge_weights([read_lse(r[:, total:], heads) for r in parts])
            row = lax.broadcasted_iota(jnp.int32, (row_count, HD), 0)
            for k in range(count):
                flag = plan_ref[2 + (shard * seq_dev + first + k) * record + record - 1]
                live = row < jnp.where(flag == 1, row_count, 1)
                for h in range(heads):
                    cols = slice(k * width + h * HD, k * width + (h + 1) * HD)
                    spot = 3 * heads * k + h
                    summed = sum(
                        r[:, cols].astype(jnp.float32) * w[:, spot : spot + 1]
                        for r, w in zip(parts, weights)
                    )
                    out_ref[k, :, h * HD : (h + 1) * HD] = jnp.where(live, summed, 0.0).astype(
                        jnp.bfloat16
                    )

        for n, r in enumerate(first_refs):
            @pl.when(one_of(shard, choice, n))
            def _(r=r):
                finish(r)

    vmem = pl.BlockSpec(memory_space=pltpu.VMEM)
    operands = [own, last_in, *first_in]
    return pl.pallas_call(
        body,
        in_specs=[pl.BlockSpec(memory_space=pltpu.SMEM)] + [vmem] * len(operands),
        out_specs=vmem,
        out_shape=pltpu.VMEM((count, row_count, width), jnp.bfloat16),
        name="merge_final",
        compiler_params=pltpu.CompilerParams(vmem_limit_bytes=16 << 20),
    )(plan, *[in_vmem(x) for x in operands])


CHUNKS = 2
BLOCK_ROWS = 512


def own_columns(core_of, queries, parts, first, count):
    _, row_count, full = queries.shape
    width = full // parts

    def body(core_ref, source, out_ref, sems):
        cols = pl.ds(pl.multiple_of(core_ref[0] * width, LANES), width)
        copies = [
            pltpu.make_async_copy(
                source.at[first + k, :, cols], out_ref.at[:, k * width : (k + 1) * width], sems.at[k]
            )
            for k in range(count)
        ]
        for c in copies:
            c.start()
        for c in copies:
            c.wait()

    return pl.pallas_call(
        body,
        in_specs=[
            pl.BlockSpec(memory_space=pltpu.SMEM),
            pl.BlockSpec(memory_space=pltpu.HBM),
        ],
        out_specs=pl.BlockSpec(memory_space=pltpu.VMEM),
        out_shape=pltpu.VMEM((row_count, count * width), queries.dtype),
        scratch_shapes=[pltpu.SemaphoreType.DMA((count,))],
        name="own_columns",
        compiler_params=pltpu.CompilerParams(vmem_limit_bytes=16 << 20),
    )(core_of, in_hbm(queries))


def place_columns(core_of, own, other, whole, *, first, seqs):
    count, row_count, width = own.shape

    def body(core_ref, own_ref, other_ref, *rest):
        out_ref, sems = rest[-2:]
        copies = []
        for n, r in enumerate((own_ref, other_ref)):
            core = core_ref[0] if n == 0 else 1 - core_ref[0]
            cols = pl.ds(pl.multiple_of(core * width, LANES), width)
            target = out_ref.at[first : first + count, :, cols]
            copies.append(pltpu.make_async_copy(r, target, sems.at[n]))
        for c in copies:
            c.start()
        for c in copies:
            c.wait()

    vmem = pl.BlockSpec(memory_space=pltpu.VMEM)
    operands = [in_vmem(own), in_vmem(other)]
    specs = [vmem, vmem]
    aliases = {}
    if whole is not None:
        operands.append(whole)
        specs.append(pl.BlockSpec(memory_space=pl.ANY))
        aliases = {3: 0}
    return pl.pallas_call(
        body,
        in_specs=[pl.BlockSpec(memory_space=pltpu.SMEM)] + specs,
        out_specs=pl.BlockSpec(memory_space=pl.ANY),
        out_shape=jax.ShapeDtypeStruct((seqs, row_count, 2 * width), own.dtype),
        scratch_shapes=[pltpu.SemaphoreType.DMA((2,))],
        input_output_aliases=aliases,
        name="place_columns",
        compiler_params=pltpu.CompilerParams(vmem_limit_bytes=16 << 20),
    )(core_of, *operands)


def queries_travel(queries, new_kv, kv_pages, page_table, cached_len, is_prefill):
    shards = lax.axis_size("seq")
    sub_count = lax.axis_size("sub")
    owners = shards * sub_count
    shard = lax.axis_index("seq")
    core = lax.axis_index("sub")
    seq_dev = queries.shape[0]
    pages_dev = kv_pages.shape[0]
    part_width = kv_pages.shape[3] // sub_count
    picks = -(-page_table.shape[1] // owners)
    record = 2 * sub_count * picks + 1
    chunk = seq_dev // CHUNKS
    firsts = [n * chunk for n in range(CHUNKS)]

    core_of = core.astype(jnp.int32)[None]
    own_queries = []
    for n in range(CHUNKS):
        own_queries.append(own_columns(core_of, queries, sub_count, firsts[n], chunk))
    _, later_pages = lax.optimization_barrier((own_queries[-1], kv_pages))
    plan = page_plan(
        page_table, cached_len, is_prefill, shard, core, pages_dev, sub_count, picks
    )

    twin = lax.dynamic_slice_in_dim(later_pages, (1 - core) * part_width, part_width, 3)
    twin_pages = lax.ppermute(twin, "sub", [(0, 1), (1, 0)])
    fresh = jnp.transpose(
        lax.dynamic_slice_in_dim(new_kv, core * part_width, part_width, 3), (2, 0, 1, 3)
    )

    whole_width = queries.shape[2] // sub_count
    common = dict(width=whole_width, seq_dev=seq_dev, picks=picks, sub_count=sub_count)

    def attend(n, sources, choice, homes, relays):
        return partial_attention(
            plan, sources, choice, homes, kv_pages, twin_pages, None, relays,
            count=chunk, first=firsts[n], **common
        )

    def move(array, pairs):
        return lax.ppermute(array, "seq", pairs)

    up = [(0, 1), (1, 2), (2, 3)]
    down = [(3, 2), (2, 1), (1, 0)]
    outward = [(2, 3), (1, 0)]
    inward = [(3, 2), (0, 1)]
    across = [(1, 2), (2, 1)]
    ends = [(3, 0), (0, 3)]
    inner = (0, 1, 1, 0)
    arrived = {}
    for n in range(CHUNKS):
        right1 = move(own_queries[n], up)
        left1 = move(own_queries[n], down)
        one, pay_right, pay_left = attend(
            n, [right1, left1], (1, 1, 0, 0), (1, 2, 1, 2), ((-1, 0, 0, 0), (1, 1, 1, -1))
        )
        right2 = move(pay_right, up)
        left2 = move(pay_left, down)
        two, pay = attend(n, [right2, left2], (1, 1, 0, 0), (2, 3, 0, 1), ((-1, 1, 0, -1),))
        third = move(pay, outward + inward)
        crossed = move(two, across)
        (three,) = attend(n, [third, left1, right1], (0, 2, 1, 0), (3, 0, 3, 0), ())
        joined = merge_pair(plan, one, third, three, chips=inner, width=whole_width)
        final = move(joined, across + ends)
        paired = merge_pair(plan, three, crossed, None, chips=inner, width=whole_width)
        home = move(paired, outward)
        arrived[n] = (final, [home, right2, left2])
    own = []
    for n in range(CHUNKS):
        (mine,) = partial_attention(
            plan, [own_queries[n]], (0,) * shards, tuple(range(shards)), kv_pages, twin_pages,
            fresh[:, firsts[n] : firsts[n] + chunk], (), count=chunk, first=firsts[n], **common
        )
        own.append(mine)
    outs = []
    for n in range(CHUNKS):
        final, firsts_in = arrived[n]
        outs.append(
            merge_final(
                plan, own[n], final, firsts_in, (0, 1, 2, 0),
                first=firsts[n], seq_dev=seq_dev, record=record, width=whole_width,
            )
        )
    whole = None
    for n in range(CHUNKS):
        other = lax.ppermute(outs[n], "sub", [(0, 1), (1, 0)])
        whole = place_columns(core_of, outs[n], other, whole, first=firsts[n], seqs=seq_dev)
    return whole


def can_travel(shards, sub_count, seq_dev, query_width, page_count):
    heads = query_width // sub_count // HD
    spread = page_count >= shards * sub_count and shards == 4 and sub_count == 2
    return spread and seq_dev % CHUNKS == 0 and 3 * heads * (seq_dev // CHUNKS) <= LANES


def solution(mesh):
    placed = (
        P(("groups", "seq"), None, "head"),
        P(("groups", "seq"), None, None, "head"),
        P(("groups", "seq", "sub"), None, None, "head"),
        P("groups", None),
        P("groups"),
        P("groups"),
    )
    shards = mesh.shape["seq"]

    def placed_map(body):
        return jax.shard_map(
            body,
            mesh=mesh,
            in_specs=placed,
            out_specs=P(("groups", "seq"), None, "head"),
            check_vma=False,
        )

    def run(queries, new_kv, kv_pages, page_table, cached_len, is_prefill):
        args = (queries, new_kv, kv_pages, page_table, cached_len, is_prefill)
        seq_dev = queries.shape[0] // (mesh.shape["groups"] * shards)
        width = queries.shape[2] // mesh.shape["head"]
        if not can_travel(shards, mesh.shape["sub"], seq_dev, width, page_table.shape[1]):
            return placed_map(pages_travel)(*args)

        return placed_map(queries_travel)(*args)

    return run
```

```python
import jax
import jax.numpy as jnp
from jax import lax
from jax.experimental import pallas as pl
from jax.experimental.pallas import tpu as pltpu
from jax.sharding import PartitionSpec as P


HD = 128
PAGE = 128


NEG_FILL = -1e30


def partial_softmax(
    query_heads, cache_keys, cache_values, cache_valid, fresh_keys, fresh_values, fresh_valid
):
    score_scale = HD ** (-0.5)
    cache_scores = (
        jnp.einsum("rkgd,nkd->kgrn", query_heads, cache_keys, preferred_element_type=jnp.float32)
        * score_scale
    )
    fresh_scores = (
        jnp.einsum("rkgd,jkd->kgrj", query_heads, fresh_keys, preferred_element_type=jnp.float32)
        * score_scale
    )
    cache_mask = cache_valid[None, None, None, :]
    fresh_mask = fresh_valid[None, None, :, :]
    peak = jnp.maximum(
        jnp.max(jnp.where(cache_mask, cache_scores, NEG_FILL), axis=-1),
        jnp.max(jnp.where(fresh_mask, fresh_scores, NEG_FILL), axis=-1),
    )
    cache_weights = jnp.where(cache_mask, jnp.exp(cache_scores - peak[..., None]), 0.0)
    fresh_weights = jnp.where(fresh_mask, jnp.exp(fresh_scores - peak[..., None]), 0.0)
    weight_sum = jnp.sum(cache_weights, axis=-1) + jnp.sum(fresh_weights, axis=-1)
    numerator = jnp.einsum(
        "kgrn,nkd->kgrd",
        cache_weights.astype(jnp.bfloat16),
        cache_values,
        preferred_element_type=jnp.float32,
    )
    numerator = numerator + jnp.einsum(
        "kgrj,jkd->kgrd",
        fresh_weights.astype(jnp.bfloat16),
        fresh_values,
        preferred_element_type=jnp.float32,
    )
    return (peak, weight_sum, numerator)


def attend_all(
    query_block, fresh_block, received, fetch_index, page_here, lengths, live_rows, causal, fresh_on
):
    kv_width = received.shape[-1]
    heads_kv = kv_width // HD
    row_count = query_block.shape[1]
    group_size = query_block.shape[2] // kv_width
    page_count = fetch_index.shape[1]
    positions = jnp.arange(page_count * PAGE, dtype=jnp.int32)

    def one_sequence(inputs):
        query_rows, fresh_rows, index_row, here_row, length, live_row = inputs
        fetched = jnp.take(received, index_row, axis=0)
        cache_keys = fetched[:, 0].reshape(page_count * PAGE, heads_kv, HD)
        cache_values = fetched[:, 1].reshape(page_count * PAGE, heads_kv, HD)
        page_mask = jnp.broadcast_to(here_row[:, None], (page_count, PAGE)).reshape(
            page_count * PAGE
        )
        cache_valid = page_mask & (positions < length)
        query_heads = query_rows.reshape(row_count, heads_kv, group_size, HD)
        fresh_keys = fresh_rows[:, 0].reshape(row_count, heads_kv, HD)
        fresh_values = fresh_rows[:, 1].reshape(row_count, heads_kv, HD)
        fresh_valid = causal & live_row[:, None] & fresh_on
        return partial_softmax(
            query_heads,
            cache_keys,
            cache_values,
            cache_valid,
            fresh_keys,
            fresh_values,
            fresh_valid,
        )

    return lax.map(
        one_sequence, (query_block, fresh_block, fetch_index, page_here, lengths, live_rows)
    )


def finish(weight_sum, numerator, live_rows):
    unused_rows = 1.0 - live_rows.astype(jnp.float32)
    attended = numerator / (weight_sum + unused_rows[:, None, None, :])[..., None]
    attended = jnp.where(live_rows[:, None, None, :, None], attended, 0.0)
    seq_dev, heads_kv, group_size, row_count, head_dim = attended.shape
    return (
        jnp.transpose(attended, (0, 3, 1, 2, 4))
        .reshape(seq_dev, row_count, heads_kv * group_size * head_dim)
        .astype(jnp.bfloat16)
    )


def pages_travel(queries, new_kv, kv_pages, page_table, cached_len, is_prefill):
    seq_shards = lax.axis_size("seq")
    sub_count = lax.axis_size("sub")
    owners = seq_shards * sub_count
    seq_index = lax.axis_index("seq")
    core_index = lax.axis_index("sub")
    owner_self = seq_index * sub_count + core_index
    seq_dev, row_count, query_width = queries.shape
    pages_dev = kv_pages.shape[0]
    kv_width = kv_pages.shape[3]
    page_count = page_table.shape[1]
    entries = seq_dev * page_count
    capacity = (entries + owners - 1) // owners
    table_rows = page_table.reshape(seq_shards, entries)
    holder = jnp.where(table_rows >= 0, table_rows // pages_dev, -1)
    slot_of = jnp.where(table_rows >= 0, table_rows % pages_dev, 0)
    owned_here = holder == owner_self
    rank_among = jnp.cumsum(owned_here.astype(jnp.int32), axis=1) - 1
    picked = owned_here[:, :, None] & (
        rank_among[:, :, None] == jnp.arange(capacity, dtype=jnp.int32)[None, None, :]
    )
    send_slots = jnp.sum(jnp.where(picked, slot_of[:, :, None], 0), axis=1).reshape(
        seq_shards * capacity
    )
    first_seq = seq_index * seq_dev
    my_table = lax.dynamic_slice_in_dim(page_table, first_seq, seq_dev, 0)
    my_lengths = lax.dynamic_slice_in_dim(cached_len, first_seq, seq_dev, 0)
    my_flags = lax.dynamic_slice_in_dim(is_prefill, first_seq, seq_dev, 0)
    flat_table = my_table.reshape(entries)
    my_holder = jnp.where(flat_table >= 0, flat_table // pages_dev, -1)
    entry_order = jnp.arange(entries, dtype=jnp.int32)
    earlier = (my_holder[:, None] == my_holder[None, :]) & (
        entry_order[None, :] < entry_order[:, None]
    )
    my_rank = jnp.sum(earlier.astype(jnp.int32), axis=1)
    row_ids = jnp.arange(row_count, dtype=jnp.int32)
    live_rows = (my_flags[:, None] == 1) | (row_ids[None, :] == 0)
    causal = row_ids[None, :] <= row_ids[:, None]
    part_width = kv_width // sub_count
    split_pages = kv_pages.reshape(pages_dev, 2, PAGE, sub_count, part_width)
    chosen = jnp.take(split_pages, send_slots, axis=0).reshape(
        seq_shards, capacity, 2, PAGE, sub_count, part_width
    )
    outgoing = jnp.moveaxis(chosen, 4, 1).reshape(owners, capacity, 2, PAGE, part_width)
    received = lax.all_to_all(
        outgoing, ("seq", "sub"), split_axis=0, concat_axis=0, tiled=True
    ).reshape(owners * capacity, 2, PAGE, part_width)
    present = flat_table >= 0
    fetch_index = jnp.where(present, my_holder * capacity + my_rank, 0)
    query_part = query_width // sub_count
    my_queries = lax.dynamic_slice_in_dim(queries, core_index * query_part, query_part, 2)
    my_fresh = lax.dynamic_slice_in_dim(new_kv, core_index * part_width, part_width, 3)
    _, weight_sum, numerator = attend_all(
        my_queries,
        my_fresh,
        received,
        fetch_index.reshape(seq_dev, page_count),
        present.reshape(seq_dev, page_count),
        my_lengths,
        live_rows,
        causal,
        core_index >= 0,
    )
    own_heads = finish(weight_sum, numerator, live_rows)
    return lax.all_gather(own_heads, "sub", axis=2, tiled=True)


LOG2E = 1.4426950408889634
LANES = 128
NO_KEY = -1e30


def page_plan(page_table, cached_len, is_prefill, shard, core, pages_dev, sub_count, picks):
    seqs, page_count = page_table.shape
    present = page_table >= 0
    owner = jnp.where(present, page_table // pages_dev, -1)
    slot = jnp.where(present, page_table % pages_dev, 0)
    page_ids = jnp.arange(page_count, dtype=jnp.int32)
    keys_here = jnp.clip(cached_len[:, None] - page_ids[None, :] * PAGE, 0, PAGE)
    before = page_ids[None, :] < page_ids[:, None]
    same = owner[:, :, None] == owner[:, None, :]
    rank = jnp.sum((same & before[None]).astype(jnp.int32), axis=2)
    cores = (core + jnp.arange(sub_count, dtype=jnp.int32)) % sub_count
    wanted = shard * sub_count + cores
    picked = (owner[:, None, None, :] == wanted[None, :, None, None]) & (
        rank[:, None, None, :] == jnp.arange(picks, dtype=jnp.int32)[None, None, :, None]
    )
    slots = jnp.sum(jnp.where(picked, slot[:, None, None, :], 0), axis=3)
    counts = jnp.sum(jnp.where(picked, keys_here[:, None, None, :], 0), axis=3)
    rows = jnp.concatenate(
        [
            slots.reshape(seqs, sub_count * picks),
            counts.reshape(seqs, sub_count * picks),
            is_prefill[:, None].astype(jnp.int32),
        ],
        axis=1,
    )
    return jnp.concatenate([jnp.stack([shard, core]).astype(jnp.int32), rows.reshape(-1)])


def lse_third(shape, heads):
    lane = lax.broadcasted_iota(jnp.int32, shape, 1)
    return lane % (3 * heads) // heads


def lse_block(lse_tile, heads):
    third = lse_third(lse_tile.shape, heads)
    high = lse_tile.astype(jnp.bfloat16)
    rest = lse_tile - high.astype(jnp.float32)
    middle = rest.astype(jnp.bfloat16)
    low = rest - middle.astype(jnp.float32)
    mixed = jnp.where(
        third == 0,
        high.astype(jnp.float32),
        jnp.where(third == 1, middle.astype(jnp.float32), low),
    )
    return mixed.astype(jnp.bfloat16)


def read_lse(block, heads):
    tile = block.astype(jnp.float32)
    return (
        tile
        + pltpu.roll(tile, LANES - heads, 1)
        + pltpu.roll(tile, LANES - 2 * heads, 1)
    )


def spread_lse(lse, heads):
    third = lse_third(lse.shape, heads)
    return jnp.where(
        third == 0,
        lse,
        jnp.where(third == 1, pltpu.roll(lse, heads, 1), pltpu.roll(lse, 2 * heads, 1)),
    )


def one_of(shard, table, value):
    found = None
    for chip, entry in enumerate(table):
        if entry == value:
            here = shard == chip
            found = here if found is None else found | here
    return found


def by_chip(shard, values):
    picked = values[0]
    for chip in range(1, len(values)):
        if values[chip] != values[chip - 1]:
            picked = jnp.where(shard >= chip, values[chip], picked)
    return picked


def partial_attention(
    plan, sources, choice, homes, pages, twin_pages, fresh, relays, *, count, width, first, seq_dev,
    picks, sub_count
):
    row_count = sources[0].shape[0]
    part_width = twin_pages.shape[3]
    heads_kv = part_width // HD
    heads = width // HD
    group = heads // heads_kv
    refs_per_seq = sub_count * picks
    record = 2 * refs_per_seq + 1
    scale = LOG2E * HD ** (-0.5)
    few = min(row_count, 16)

    def entry(plan_ref, k, column):
        home = by_chip(plan_ref[0], homes)
        return plan_ref[2 + (home * seq_dev + first + k) * record + column]

    total = count * width

    def body(plan_ref, *rest):
        query_refs = rest[: len(sources)]
        pages_hbm, twin_hbm = rest[len(sources) : len(sources) + 2]
        fresh_ref = rest[len(sources) + 2] if fresh is not None else None
        query_ref, result_ref, page_buf, sems = rest[-4:]
        out_ref = rest[-5 - len(relays)]
        relay_refs = rest[-4 - len(relays) : -4]
        shard = plan_ref[0]
        mine = pl.ds(pl.multiple_of(plan_ref[1] * part_width, LANES), part_width)

        def page_copy(k, n):
            slot = entry(plan_ref, k, n)
            source = pages_hbm.at[slot, :, :, mine] if n < picks else twin_hbm.at[slot]
            return pltpu.make_async_copy(source, page_buf.at[k, n], sems.at[k, n])

        for k in range(count):
            for n in range(refs_per_seq):
                page_copy(k, n).start()

        def one(k, carry):
            attend_one(k)
            return carry

        def attend_one(k):
            counts = [entry(plan_ref, k, refs_per_seq + n) for n in range(refs_per_seq)]
            flag = entry(plan_ref, k, 2 * refs_per_seq)
            for j in range(count):
                for n in range(len(sources)):
                    @pl.when((k == j) & one_of(shard, choice, n))
                    def _(n=n, j=j):
                        query_ref[...] = query_refs[n][:, j * width : (j + 1) * width]

            for n in range(refs_per_seq):
                page_copy(k, n).wait()

            @pl.when(flag == 1)
            def _():
                attend(k, counts, row_count, row_count)

            @pl.when(flag != 1)
            def _():
                attend(k, counts, few, 1)
                if few < row_count:
                    result_ref[few:, :] = jnp.zeros((row_count - few, width), jnp.bfloat16)

            for j in range(count):
                @pl.when(k == j)
                def _(j=j):
                    out_ref[:, j * width : (j + 1) * width] = result_ref[...]

        def attend(k, counts, rows, live_rows):
            lane = lax.broadcasted_iota(jnp.int32, (rows, LANES), 1)
            tile = jnp.zeros((rows, LANES), jnp.float32)
            start = k * (3 * heads)
            per_block = max(1, min(group, BLOCK_ROWS // rows))
            stacked = per_block * rows
            key_lane = lax.broadcasted_iota(jnp.int32, (stacked, PAGE), 1)
            for h in range(heads_kv):
                cols = slice(h * HD, (h + 1) * HD)
                keys = jnp.concatenate([page_buf[k, n, 0, :, cols] for n in range(refs_per_seq)], axis=0)
                values = jnp.concatenate([page_buf[k, n, 1, :, cols] for n in range(refs_per_seq)], axis=0)
                for g0 in range(0, group, per_block):
                    base = h * group + g0
                    q = jnp.concatenate(
                        [
                            query_ref[:rows, (base + g) * HD : (base + g + 1) * HD]
                            for g in range(per_block)
                        ],
                        axis=0,
                    )
                    s = lax.dot_general(
                        q, keys, (((1,), (1,)), ((), ())), preferred_element_type=jnp.float32
                    )
                    scores = [
                        jnp.where(
                            key_lane < counts[n], s[:, n * PAGE : (n + 1) * PAGE] * scale, NO_KEY
                        )
                        for n in range(refs_per_seq)
                    ]
                    peak = scores[0]
                    for x in scores[1:]:
                        peak = jnp.maximum(peak, x)
                    peak = jnp.max(peak, axis=1, keepdims=True)
                    if fresh is not None:
                        s = lax.dot_general(
                            q,
                            fresh_ref[0, k, :, cols],
                            (((1,), (1,)), ((), ())),
                            preferred_element_type=jnp.float32,
                        )
                        row = lax.broadcasted_iota(jnp.int32, (stacked, row_count), 0) % rows
                        col = lax.broadcasted_iota(jnp.int32, (stacked, row_count), 1)
                        new_scores = jnp.where(
                            (col <= row) & (col < live_rows), s * scale, NO_KEY
                        )
                        peak = jnp.maximum(peak, jnp.max(new_scores, axis=1, keepdims=True))
                    weights = [jnp.exp2(x - peak) for x in scores]
                    sums = weights[0]
                    for w in weights[1:]:
                        sums = sums + w
                    weight_sum = jnp.sum(sums, axis=1, keepdims=True)
                    numerator = lax.dot_general(
                        jnp.concatenate([w.astype(jnp.bfloat16) for w in weights], axis=1),
                        values,
                        (((1,), (0,)), ((), ())),
                        preferred_element_type=jnp.float32,
                    )
                    if fresh is not None:
                        w = jnp.exp2(new_scores - peak)
                        weight_sum = weight_sum + jnp.sum(w, axis=1, keepdims=True)
                        numerator = numerator + lax.dot_general(
                            w.astype(jnp.bfloat16),
                            fresh_ref[1, k, :, cols],
                            (((1,), (0,)), ((), ())),
                            preferred_element_type=jnp.float32,
                        )
                    attended = (numerator / weight_sum).astype(jnp.bfloat16)
                    lse = peak + jnp.log2(weight_sum)
                    for g in range(per_block):
                        head = base + g
                        part = slice(g * rows, (g + 1) * rows)
                        result_ref[:rows, head * HD : (head + 1) * HD] = attended[part]
                        spot = lane - start - head
                        spots = (spot == 0) | (spot == heads) | (spot == 2 * heads)
                        tile = jnp.where(spots, lse[part], tile)
            here = (lane >= start) & (lane < start + 3 * heads)
            before = out_ref[:rows, total:].astype(jnp.float32)
            block = lse_block(tile, heads).astype(jnp.float32)
            out_ref[:rows, total:] = jnp.where(here, block, before).astype(jnp.bfloat16)

        out_ref[:, total:] = jnp.zeros((row_count, LANES), jnp.bfloat16)
        for relay, relay_ref in zip(relays, relay_refs):
            for n in range(len(sources)):
                if n in relay:
                    @pl.when(one_of(shard, relay, n))
                    def _(n=n, relay_ref=relay_ref):
                        relay_ref[:, :total] = query_refs[n][:, :total]
        lax.fori_loop(0, count, one, 0)
        for relay, relay_ref in zip(relays, relay_refs):
            @pl.when(one_of(shard, relay, -1))
            def _(relay_ref=relay_ref):
                relay_ref[...] = out_ref[...]

    vmem = pl.BlockSpec(memory_space=pltpu.VMEM)
    hbm = pl.BlockSpec(memory_space=pltpu.HBM)
    operands = [in_vmem(x) for x in sources] + [in_hbm(pages), in_hbm(twin_pages)]
    in_specs = [vmem] * len(sources) + [hbm, hbm]
    if fresh is not None:
        operands.append(fresh)
        in_specs.append(vmem)
    outs = 1 + len(relays)
    return pl.pallas_call(
        body,
        in_specs=[pl.BlockSpec(memory_space=pltpu.SMEM)] + in_specs,
        out_specs=[vmem] * outs,
        out_shape=[pltpu.VMEM((row_count, total + LANES), jnp.bfloat16)] * outs,
        scratch_shapes=[
            pltpu.VMEM((row_count, width), jnp.bfloat16),
            pltpu.VMEM((row_count, width), jnp.bfloat16),
            pltpu.VMEM((count, refs_per_seq, 2, PAGE, part_width), jnp.bfloat16),
            pltpu.SemaphoreType.DMA((count, refs_per_seq)),
        ],
        name="partial_attention",
        compiler_params=pltpu.CompilerParams(vmem_limit_bytes=24 << 20),
        cost_estimate=pl.CostEstimate(
            flops=count * heads * row_count * refs_per_seq * PAGE * HD * 4,
            bytes_accessed=count * row_count * width * 8,
            transcendentals=count * heads * row_count * refs_per_seq * PAGE,
        ),
    )(plan, *operands)


def in_hbm(array):
    return pltpu.with_memory_space_constraint(array, pltpu.HBM)


def in_vmem(array):
    return pltpu.with_memory_space_constraint(array, pltpu.VMEM)


def merge_weights(lses):
    peak = lses[0]
    for lse in lses[1:]:
        peak = jnp.maximum(peak, lse)
    weights = [jnp.exp2(lse - peak) for lse in lses]
    total = weights[0]
    for w in weights[1:]:
        total = total + w
    return [w / total for w in weights], peak + jnp.log2(total)


def merge_pair(plan, mine, incoming, other, *, chips, width):
    total = mine.shape[1] - LANES
    heads = width // HD
    inputs = [mine, incoming] + ([other] if other is not None else [])

    def body(plan_ref, *rest):
        out_ref = rest[len(inputs)]
        here = one_of(plan_ref[0], chips, 1)

        @pl.when(here)
        def _():
            parts = rest[:2]
            weights, lse = merge_weights([read_lse(r[:, total:], heads) for r in parts])
            for k in range(total // width):
                for h in range(heads):
                    cols = slice(k * width + h * HD, k * width + (h + 1) * HD)
                    spot = 3 * heads * k + h
                    out_ref[:, cols] = sum(
                        r[:, cols].astype(jnp.float32) * w[:, spot : spot + 1]
                        for r, w in zip(parts, weights)
                    ).astype(jnp.bfloat16)
            out_ref[:, total:] = lse_block(spread_lse(lse, heads), heads)

        if other is not None:
            @pl.when(jnp.logical_not(here))
            def _():
                out_ref[...] = rest[2][...]

    vmem = pl.BlockSpec(memory_space=pltpu.VMEM)
    return pl.pallas_call(
        body,
        in_specs=[pl.BlockSpec(memory_space=pltpu.SMEM)] + [vmem] * len(inputs),
        out_specs=vmem,
        out_shape=pltpu.VMEM(mine.shape, jnp.bfloat16),
        name="merge_pair",
        compiler_params=pltpu.CompilerParams(vmem_limit_bytes=16 << 20),
    )(plan, *[in_vmem(x) for x in inputs])


def merge_final(plan, own, last_in, first_in, choice, *, first, seq_dev, record, width):
    row_count, full = last_in.shape
    total = full - LANES
    count = total // width
    heads = width // HD

    def body(plan_ref, own_ref, last_ref, *rest):
        first_refs = rest[: len(first_in)]
        out_ref = rest[len(first_in)]
        shard = plan_ref[0]

        def finish(first_ref):
            parts = [own_ref, last_ref, first_ref]
            weights, _ = merge_weights([read_lse(r[:, total:], heads) for r in parts])
            row = lax.broadcasted_iota(jnp.int32, (row_count, HD), 0)
            for k in range(count):
                flag = plan_ref[2 + (shard * seq_dev + first + k) * record + record - 1]
                live = row < jnp.where(flag == 1, row_count, 1)
                for h in range(heads):
                    cols = slice(k * width + h * HD, k * width + (h + 1) * HD)
                    spot = 3 * heads * k + h
                    summed = sum(
                        r[:, cols].astype(jnp.float32) * w[:, spot : spot + 1]
                        for r, w in zip(parts, weights)
                    )
                    out_ref[k, :, h * HD : (h + 1) * HD] = jnp.where(live, summed, 0.0).astype(
                        jnp.bfloat16
                    )

        for n, r in enumerate(first_refs):
            @pl.when(one_of(shard, choice, n))
            def _(r=r):
                finish(r)

    vmem = pl.BlockSpec(memory_space=pltpu.VMEM)
    operands = [own, last_in, *first_in]
    return pl.pallas_call(
        body,
        in_specs=[pl.BlockSpec(memory_space=pltpu.SMEM)] + [vmem] * len(operands),
        out_specs=vmem,
        out_shape=pltpu.VMEM((count, row_count, width), jnp.bfloat16),
        name="merge_final",
        compiler_params=pltpu.CompilerParams(vmem_limit_bytes=16 << 20),
    )(plan, *[in_vmem(x) for x in operands])


CHUNKS = 2
BLOCK_ROWS = 512


def own_columns(core_of, queries, parts, first, count):
    _, row_count, full = queries.shape
    width = full // parts

    def body(core_ref, source, out_ref, sems):
        cols = pl.ds(pl.multiple_of(core_ref[0] * width, LANES), width)
        copies = [
            pltpu.make_async_copy(
                source.at[first + k, :, cols], out_ref.at[:, k * width : (k + 1) * width], sems.at[k]
            )
            for k in range(count)
        ]
        for c in copies:
            c.start()
        for c in copies:
            c.wait()

    return pl.pallas_call(
        body,
        in_specs=[
            pl.BlockSpec(memory_space=pltpu.SMEM),
            pl.BlockSpec(memory_space=pltpu.HBM),
        ],
        out_specs=pl.BlockSpec(memory_space=pltpu.VMEM),
        out_shape=pltpu.VMEM((row_count, count * width), queries.dtype),
        scratch_shapes=[pltpu.SemaphoreType.DMA((count,))],
        name="own_columns",
        compiler_params=pltpu.CompilerParams(vmem_limit_bytes=16 << 20),
    )(core_of, in_hbm(queries))


def place_columns(core_of, own, other, whole, *, first, seqs):
    count, row_count, width = own.shape

    def body(core_ref, own_ref, other_ref, *rest):
        out_ref, sems = rest[-2:]
        copies = []
        for n, r in enumerate((own_ref, other_ref)):
            core = core_ref[0] if n == 0 else 1 - core_ref[0]
            cols = pl.ds(pl.multiple_of(core * width, LANES), width)
            target = out_ref.at[first : first + count, :, cols]
            copies.append(pltpu.make_async_copy(r, target, sems.at[n]))
        for c in copies:
            c.start()
        for c in copies:
            c.wait()

    vmem = pl.BlockSpec(memory_space=pltpu.VMEM)
    operands = [in_vmem(own), in_vmem(other)]
    specs = [vmem, vmem]
    aliases = {}
    if whole is not None:
        operands.append(whole)
        specs.append(pl.BlockSpec(memory_space=pl.ANY))
        aliases = {3: 0}
    return pl.pallas_call(
        body,
        in_specs=[pl.BlockSpec(memory_space=pltpu.SMEM)] + specs,
        out_specs=pl.BlockSpec(memory_space=pl.ANY),
        out_shape=jax.ShapeDtypeStruct((seqs, row_count, 2 * width), own.dtype),
        scratch_shapes=[pltpu.SemaphoreType.DMA((2,))],
        input_output_aliases=aliases,
        name="place_columns",
        compiler_params=pltpu.CompilerParams(vmem_limit_bytes=16 << 20),
    )(core_of, *operands)


def queries_travel(queries, new_kv, kv_pages, page_table, cached_len, is_prefill):
    shards = lax.axis_size("seq")
    sub_count = lax.axis_size("sub")
    owners = shards * sub_count
    shard = lax.axis_index("seq")
    core = lax.axis_index("sub")
    seq_dev = queries.shape[0]
    pages_dev = kv_pages.shape[0]
    part_width = kv_pages.shape[3] // sub_count
    picks = -(-page_table.shape[1] // owners)
    record = 2 * sub_count * picks + 1
    chunk = seq_dev // CHUNKS
    firsts = [n * chunk for n in range(CHUNKS)]

    core_of = core.astype(jnp.int32)[None]
    own_queries = []
    for n in range(CHUNKS):
        own_queries.append(own_columns(core_of, queries, sub_count, firsts[n], chunk))
    _, later_pages = lax.optimization_barrier((own_queries[-1], kv_pages))
    plan = page_plan(
        page_table, cached_len, is_prefill, shard, core, pages_dev, sub_count, picks
    )

    twin = lax.dynamic_slice_in_dim(later_pages, (1 - core) * part_width, part_width, 3)
    twin_pages = lax.ppermute(twin, "sub", [(0, 1), (1, 0)])
    fresh = jnp.transpose(
        lax.dynamic_slice_in_dim(new_kv, core * part_width, part_width, 3), (2, 0, 1, 3)
    )

    whole_width = queries.shape[2] // sub_count
    common = dict(width=whole_width, seq_dev=seq_dev, picks=picks, sub_count=sub_count)

    def attend(n, sources, choice, homes, relays):
        return partial_attention(
            plan, sources, choice, homes, kv_pages, twin_pages, None, relays,
            count=chunk, first=firsts[n], **common
        )

    def move(array, pairs):
        return lax.ppermute(array, "seq", pairs)

    outer = [(0, 1), (1, 0), (2, 3), (3, 2)]
    across = [(1, 2), (2, 1)]
    ends = [(3, 0), (0, 3)]
    inner = (0, 1, 1, 0)
    relay = ((-1, 1, 1, -1),)
    arrived = {}
    for n in range(CHUNKS):
        middle1 = move(own_queries[n], across)
        outer1 = move(own_queries[n], outer)
        middle2 = move(outer1, across)
        one, pay = attend(n, [outer1, middle1], inner, (1, 2, 1, 2), relay)
        outer2 = move(pay, outer)
        two, pay = attend(n, [outer2, middle2], inner, (2, 3, 0, 1), relay)
        crossed = move(two, across)
        outer3 = move(pay, outer)
        (three,) = attend(n, [outer3, outer1], inner, (3, 0, 3, 0), ())
        joined = merge_pair(plan, one, outer3, three, chips=inner, width=whole_width)
        final = move(joined, across + ends)
        paired = merge_pair(plan, three, crossed, None, chips=inner, width=whole_width)
        home = move(paired, [(1, 0), (2, 3)])
        arrived[n] = (final, [home, outer2])
    own = []
    for n in range(CHUNKS):
        (mine,) = partial_attention(
            plan, [own_queries[n]], (0,) * shards, tuple(range(shards)), kv_pages, twin_pages,
            fresh[:, firsts[n] : firsts[n] + chunk], (), count=chunk, first=firsts[n], **common
        )
        own.append(mine)
    outs = []
    for n in range(CHUNKS):
        final, firsts_in = arrived[n]
        outs.append(
            merge_final(
                plan, own[n], final, firsts_in, inner,
                first=firsts[n], seq_dev=seq_dev, record=record, width=whole_width,
            )
        )
    whole = None
    for n in range(CHUNKS):
        other = lax.ppermute(outs[n], "sub", [(0, 1), (1, 0)])
        whole = place_columns(core_of, outs[n], other, whole, first=firsts[n], seqs=seq_dev)
    return whole


def can_travel(shards, sub_count, seq_dev, query_width, page_count):
    heads = query_width // sub_count // HD
    spread = page_count >= shards * sub_count and shards == 4 and sub_count == 2
    return spread and seq_dev % CHUNKS == 0 and 3 * heads * (seq_dev // CHUNKS) <= LANES


def solution(mesh):
    placed = (
        P(("groups", "seq"), None, "head"),
        P(("groups", "seq"), None, None, "head"),
        P(("groups", "seq", "sub"), None, None, "head"),
        P("groups", None),
        P("groups"),
        P("groups"),
    )
    shards = mesh.shape["seq"]

    def placed_map(body):
        return jax.shard_map(
            body,
            mesh=mesh,
            in_specs=placed,
            out_specs=P(("groups", "seq"), None, "head"),
            check_vma=False,
        )

    def run(queries, new_kv, kv_pages, page_table, cached_len, is_prefill):
        args = (queries, new_kv, kv_pages, page_table, cached_len, is_prefill)
        seq_dev = queries.shape[0] // (mesh.shape["groups"] * shards)
        width = queries.shape[2] // mesh.shape["head"]
        if not can_travel(shards, mesh.shape["sub"], seq_dev, width, page_table.shape[1]):
            return placed_map(pages_travel)(*args)

        return placed_map(queries_travel)(*args)

    return run
```
